32 devices in a mesh: seq: 4 (over y, x), fsdp: 8 (over z, core).
Axes of the slice: x: 2, y: 2, z: 4, core: 2. Of those that a mesh axis runs over, the one named last changes fastest.
Arguments:
- block_input: bfloat16 [2, 8, 1024, 2048], P(None, 'fsdp', 'seq'), may hold values from -6 to 6
- out_grad: bfloat16 [2, 8, 1024, 2048], P(None, 'fsdp', 'seq'), may hold values from -6 to 6
- query_proj: bfloat16 [2048, 2048], P('fsdp', 'seq'), may hold values from -0.125 to 0.125
- key_projection: bfloat16 [2048, 1024], P('fsdp', 'seq'), may hold values from -0.125 to 0.125
- value_projection: bfloat16 [2048, 1024], P('fsdp', 'seq'), may hold values from -0.125 to 0.125
- outgate_proj: bfloat16 [2048, 2048], P('fsdp', 'seq'), may hold values from -0.125 to 0.125
- output_proj: bfloat16 [2048, 2048], P('seq', 'fsdp'), may hold values from -1 to 1
- ffgate_proj: bfloat16 [2048, 6144], P('fsdp', 'seq'), may hold values from -0.125 to 0.125
- ffup_proj: bfloat16 [2048, 6144], P('fsdp', 'seq'), may hold values from -0.125 to 0.125
- ffdown_proj: bfloat16 [6144, 2048], P('seq', 'fsdp'), may hold values from -0.078125 to 0.078125
- attn_gain: float32 [2048], replicated, may hold values from 0.5 to 1.5
- ffn_gain: float32 [2048], replicated, may hold values from 0.5 to 1.5
- query_gain: float32 [128], replicated, may hold values from 0.1 to 1.9
- key_gain: float32 [128], replicated, may hold values from 0.1 to 1.9
- piece_order: int32 [2, 8, 8], P(None, 'fsdp'), may hold values from 0 to 7, each once within a row
- doc_ids: int32 [2, 8, 1024], P(None, 'fsdp'), may hold values from 0 to 3, never falling along the last dimension, each value on 1 to 512 neighbouring positions
Outputs:
- block_output: bfloat16 [2, 8, 1024, 2048], P(None, 'fsdp', 'seq')
- input_grad: bfloat16 [2, 8, 1024, 2048], P(None, 'fsdp', 'seq')
- query_grad: float32 [2048, 2048], P('fsdp', 'seq')
- key_grad: float32 [2048, 1024], P('fsdp', 'seq')
- value_grad: float32 [2048, 1024], P('fsdp', 'seq')
- outgate_grad: float32 [2048, 2048], P('fsdp', 'seq')
- output_grad: float32 [2048, 2048], P('seq', 'fsdp')
- ffgate_grad: float32 [2048, 6144], P('fsdp', 'seq')
- ffup_grad: float32 [2048, 6144], P('fsdp', 'seq')
- ffdown_grad: float32 [6144, 2048], P('seq', 'fsdp')
- attn_gain_grad: float32 [2048], replicated
- ffn_gain_grad: float32 [2048], replicated
- query_gain_grad: float32 [128], replicated
- key_gain_grad: float32 [128], replicated
The draws below stay inside these ranges and needn't reach their ends.
Inputs may be any that keep to these rules, and one draw needn't show every extreme that they name: For each sequence, piece_order is a permutation of the 8 first pieces. `doc_ids`: document numbers never fall along a sequence's first order; each of the 4 documents covers 1 to 512 positions, and one covers exactly 512.
All inputs are finite; a program needn't handle non-finite values.
Results may differ from the reference program's by a relative error of at most 0.02.
Values may be sent and summed in bfloat16 or wider, within the bound.
A program may use at most 320 MiB of HBM per device.

```python
import math
import jax
import jax.numpy as jnp
import numpy as np
from jax import lax

MODEL_WIDTH = 2048
QUERY_HEADS = 16
KEY_VALUE_HEADS = 8
HEAD_SIZE = 128
FF = 6144
LEN = 1024
MB = 2
DOCS = 4
BATCH = 8
N_SEQ = 4


def steps_of(rng, extent, pieces, least, largest):
    level, own = 1.0, jax.random.fold_in(rng, 6)
    for axis_at, shards_of in pieces:
        heights = jnp.exp(jax.random.uniform(jax.random.fold_in(own, axis_at), (shards_of,), jnp.float32, least / len(pieces), largest / len(pieces)))
        level = level * jnp.repeat(heights, extent[axis_at] // shards_of).reshape([-1 if axis == axis_at else 1 for axis in range(len(extent))])
    return level


def split_up(amount, total, limit, slope):
    loads = [(1 << 20) // math.isqrt(standing ** slope) + 1 for standing in range(2, amount + 1)]
    surplus, holding = total - limit - (amount - 1), [1] * (amount - 1)
    while surplus > 0:
        free = [i for i in range(amount - 1) if holding[i] < limit]
        mass, budget = sum([loads[i] for i in free]), surplus
        for i in free:
            more = min(limit - holding[i], max(1, budget * loads[i] // mass), surplus)
            holding[i] = holding[i] + more
            surplus = surplus - more
    return np.array([limit] + holding)


def uneven_parts(own_key, amount, total, most, slope):
    if amount == 2:
        one = jax.random.randint(own_key, (), max(1, total - most), min(most, total - 1) + 1)
        return jnp.stack([one, total - one])
    sizes = jnp.asarray(split_up(amount, total, most, slope), jnp.int32)
    couples = (amount - 1) // 2
    giver, taker = sizes[1:1 + 2 * couples:2], sizes[2:2 + 2 * couples:2]
    slack = jnp.minimum(giver - 1, most - taker)
    shifted = jax.random.randint(jax.random.fold_in(own_key, 1), (couples,), 0, 1 << 20) % (slack + 1)
    sizes = sizes.at[1:1 + 2 * couples:2].set(giver - shifted).at[2:2 + 2 * couples:2].set(taker + shifted)
    return sizes[jax.random.permutation(jax.random.fold_in(own_key, 2), amount)]


def normal_values(stream_key, dims, deviation, limit, pieces=(), held_as=jnp.bfloat16):
    values = jax.random.normal(stream_key, dims, jnp.float32) * deviation
    if len(pieces) > 0:
        values = steps_of(stream_key, dims, pieces, -0.22, 0.18) * values
    return jnp.clip(values, min=-limit, max=limit).astype(held_as)


def setup_inputs(seed: int = 0) -> dict:
    key_of = jax.random.split(jax.random.key(seed), 17)
    return {
        "block_input": normal_values(key_of[0], (MB, BATCH, LEN, MODEL_WIDTH), 1.0, 6.0, ((1, 8), (2, 4))),
        "out_grad": normal_values(key_of[1], (MB, BATCH, LEN, MODEL_WIDTH), 1.0, 6.0, ((1, 8), (2, 4))),
        "query_proj": normal_values(key_of[2], (MODEL_WIDTH, QUERY_HEADS * HEAD_SIZE), MODEL_WIDTH ** -0.5, 0.125, ((0, 8), (1, 4))),
        "key_projection": normal_values(key_of[3], (MODEL_WIDTH, KEY_VALUE_HEADS * HEAD_SIZE), MODEL_WIDTH ** -0.5, 0.125, ((0, 8), (1, 4))),
        "value_projection": normal_values(key_of[4], (MODEL_WIDTH, KEY_VALUE_HEADS * HEAD_SIZE), MODEL_WIDTH ** -0.5, 0.125, ((0, 8), (1, 4))),
        "outgate_proj": normal_values(key_of[5], (MODEL_WIDTH, QUERY_HEADS * HEAD_SIZE), MODEL_WIDTH ** -0.5, 0.125, ((0, 8), (1, 4))),
        "output_proj": normal_values(key_of[6], (QUERY_HEADS * HEAD_SIZE, MODEL_WIDTH), (QUERY_HEADS * HEAD_SIZE // 64) ** -0.5, 1.0, ((0, 4), (1, 8))),
        "ffgate_proj": normal_values(key_of[7], (MODEL_WIDTH, FF), MODEL_WIDTH ** -0.5, 0.125, ((0, 8), (1, 4))),
        "ffup_proj": normal_values(key_of[8], (MODEL_WIDTH, FF), MODEL_WIDTH ** -0.5, 0.125, ((0, 8), (1, 4))),
        "ffdown_proj": normal_values(key_of[9], (FF, MODEL_WIDTH), FF ** -0.5, 0.078125, ((0, 4), (1, 8))),
        "attn_gain": jnp.clip(1.0 + 0.1 * jax.random.normal(key_of[10], (MODEL_WIDTH,), jnp.float32), 0.5, 1.5),
        "ffn_gain": jnp.clip(1.0 + 0.1 * jax.random.normal(key_of[11], (MODEL_WIDTH,), jnp.float32), 0.5, 1.5),
        "query_gain": jnp.clip(1.0 + 0.18 * jax.random.normal(key_of[12], (HEAD_SIZE,), jnp.float32), 0.1, 1.9),
        "key_gain": jnp.clip(1.0 + 0.18 * jax.random.normal(key_of[13], (HEAD_SIZE,), jnp.float32), 0.1, 1.9),
        "piece_order": jax.vmap(lambda own: jax.random.permutation(own, 2 * N_SEQ))(jax.random.split(key_of[14], MB * BATCH)).reshape((MB, BATCH, 2 * N_SEQ)).astype(jnp.int32),
        "doc_ids": jax.vmap(lambda own: jnp.searchsorted(jnp.cumsum(uneven_parts(own, DOCS, LEN, LEN // 2, 2)), jnp.arange(LEN), side="right"))(jax.random.split(key_of[15], MB * BATCH)).reshape((MB, BATCH, LEN)).astype(jnp.int32),
    }


EPSILON = 1e-06
ROPE_BASE = 5000000.0
NEG_LARGE = -1e+30
HIGHEST = lax.Precision.HIGHEST

@jax.custom_vjp
def to_lower_precision(v):
    return lax.optimization_barrier(v.astype(jnp.bfloat16)).astype(jnp.float32)

@jax.custom_vjp
def lower_precision_backward(v):
    return v

def low_keep(v):
    return (to_lower_precision(v), None)

def low_pass(kept, grad):
    return (grad,)

def back_keep(v):
    return (v, None)

def back_low(kept, grad):
    return (to_lower_precision(grad),)
to_lower_precision.defvjp(low_keep, low_pass)
lower_precision_backward.defvjp(back_keep, back_low)

def matrix_product(left, right):
    return jnp.dot(left, right, precision=HIGHEST)

def root_mean_square_norm(values, gain):
    return values * lax.rsqrt(lax.optimization_barrier(jnp.mean(values * values, axis=-1, keepdims=True)) + EPSILON) * gain

def rope_tables(positions, head_dim):
    half_dim = head_dim // 2
    inverse = jnp.exp(-math.log(ROPE_BASE) * 2.0 * jnp.arange(half_dim, dtype=jnp.float32) / head_dim)
    angles = positions.astype(jnp.float32)[:, None] * inverse[None, :]
    cosines = jnp.cos(angles)
    sines = jnp.sin(angles)
    return (jnp.concatenate([cosines, cosines], -1), jnp.concatenate([sines, sines], -1))

def apply_rotary(values, cosine_lookup, sine_lookup):
    half_dim = values.shape[-1] // 2
    turned = jnp.concatenate([-values[..., half_dim:], values[..., :half_dim]], -1)
    return values * cosine_lookup + turned * sine_lookup

def layer(inputs, weights, positions, doc_rows):
    query_w, key_weight_matrix, value_weight_matrix, outgate_w, output_w, ffgate_w, ffup_w, ffdown_w, attn_g, ffn_g, query_norm_gain, key_g = weights
    sequence_length = inputs.shape[0]
    heads_per_group = QUERY_HEADS // KEY_VALUE_HEADS
    first_normalized = to_lower_precision(root_mean_square_norm(inputs, attn_g))
    query_before_rotation = lower_precision_backward(matrix_product(first_normalized, query_w)).reshape(sequence_length, QUERY_HEADS, HEAD_SIZE)
    key_before_rotation = lower_precision_backward(matrix_product(first_normalized, key_weight_matrix)).reshape(sequence_length, KEY_VALUE_HEADS, HEAD_SIZE)
    value_row_block = to_lower_precision(lower_precision_backward(matrix_product(first_normalized, value_weight_matrix))).reshape(sequence_length, KEY_VALUE_HEADS, HEAD_SIZE)
    gate_pre = lower_precision_backward(matrix_product(first_normalized, outgate_w))
    cosine_lookup, sine_lookup = rope_tables(positions, HEAD_SIZE)
    cosine_lookup = cosine_lookup[:, None, :]
    sine_lookup = sine_lookup[:, None, :]
    query_row_block = to_lower_precision(apply_rotary(root_mean_square_norm(query_before_rotation, query_norm_gain), cosine_lookup, sine_lookup)).reshape(sequence_length, KEY_VALUE_HEADS, heads_per_group, HEAD_SIZE)
    key_rows = to_lower_precision(apply_rotary(root_mean_square_norm(key_before_rotation, key_g), cosine_lookup, sine_lookup))
    raw_scores = lower_precision_backward(jnp.einsum('qhgd,khd->hgqk', query_row_block, key_rows, precision=HIGHEST))
    scores = raw_scores * HEAD_SIZE ** (-0.5)
    visible = (positions[None, :] <= positions[:, None]) & (doc_rows[None, :] == doc_rows[:, None])
    scores = jnp.where(visible, scores, NEG_LARGE)
    highest = lax.optimization_barrier(jnp.max(scores, axis=-1, keepdims=True))
    exponents = jnp.exp(scores - highest)
    probs = exponents / lax.optimization_barrier(jnp.sum(exponents, axis=-1, keepdims=True))
    prob_low = to_lower_precision(probs)
    attn_out = jnp.einsum('hgqk,khd->qhgd', prob_low, value_row_block, precision=HIGHEST).reshape(sequence_length, QUERY_HEADS * HEAD_SIZE)
    attn_out = lower_precision_backward(attn_out)
    gated = to_lower_precision(attn_out * jax.nn.sigmoid(gate_pre))
    middle = inputs + lower_precision_backward(matrix_product(gated, output_w))
    normed_two = to_lower_precision(root_mean_square_norm(middle, ffn_g))
    gate_ffn = lower_precision_backward(matrix_product(normed_two, ffgate_w))
    up_ffn = lower_precision_backward(matrix_product(normed_two, ffup_w))
    hidden = to_lower_precision(jax.nn.silu(gate_ffn) * up_ffn)
    return middle + lower_precision_backward(matrix_product(hidden, ffdown_w))

def reference(block_input, out_grad, query_proj, key_projection, value_projection, outgate_proj, output_proj, ffgate_proj, ffup_proj, ffdown_proj, attn_gain, ffn_gain, query_gain, key_gain, piece_order, doc_ids):
    params = tuple((weight.astype(jnp.float32) for weight in (query_proj, key_projection, value_projection, outgate_proj, output_proj, ffgate_proj, ffup_proj, ffdown_proj, attn_gain, ffn_gain, query_gain, key_gain)))
    total_seqs = MB * BATCH
    inputs = block_input.reshape(total_seqs, LEN, MODEL_WIDTH)
    cotangents = out_grad.reshape(total_seqs, LEN, MODEL_WIDTH)
    orders = piece_order.reshape(total_seqs, 2 * N_SEQ).astype(jnp.int32)
    documents = doc_ids.reshape(total_seqs, LEN).astype(jnp.int32)
    piece_len = LEN // (2 * N_SEQ)

    def one_sequence(carry, item):
        inputs_one, cot_one, order_one, docs_one = item
        positions = (order_one[:, None] * piece_len + jnp.arange(piece_len, dtype=jnp.int32)[None, :]).reshape(LEN).astype(jnp.int32)
        doc_rows = docs_one[positions]

        def forward(inputs_f, *weights):
            return layer(inputs_f, weights, positions, doc_rows)
        result, pullback = jax.vjp(forward, inputs_one.astype(jnp.float32), *params)
        grads = pullback(cot_one.astype(jnp.float32))
        carry = tuple((total_part + fresh_part for total_part, fresh_part in zip(carry, grads[1:])))
        return (carry, (result.astype(jnp.bfloat16), grads[0].astype(jnp.bfloat16)))
    zeros = tuple((jnp.zeros(param.shape, jnp.float32) for param in params))
    sums, (outputs, in_grads) = lax.scan(one_sequence, zeros, (inputs, cotangents, orders, documents))
    return (outputs.reshape(MB, BATCH, LEN, MODEL_WIDTH), in_grads.reshape(MB, BATCH, LEN, MODEL_WIDTH), sums[0], sums[1], sums[2], sums[3], sums[4], sums[5], sums[6], sums[7], sums[8], sums[9], sums[10], sums[11])
```

```python
import math

import jax
import jax.numpy as jnp
from jax import lax
from jax.sharding import PartitionSpec as P

HEAD_SIZE = 128


EPSILON = 1e-06
ROPE_BASE = 5000000.0
NEG_LARGE = -1e30


def rms_scale(values):
    return lax.rsqrt(jnp.mean(values * values, axis=-1, keepdims=True) + EPSILON)


def rms_back(grad_out, normed, scales, gain):
    scaled_grad = grad_out * gain
    return scales * (scaled_grad - normed * jnp.mean(scaled_grad * normed, axis=-1, keepdims=True))


def rope_tables(positions, head_dim):
    half_dim = head_dim // 2
    inverse = jnp.exp(
        -math.log(ROPE_BASE) * 2.0 * jnp.arange(half_dim, dtype=jnp.float32) / head_dim
    )
    angles = positions.astype(jnp.float32)[:, None] * inverse[None, :]
    cosines = jnp.cos(angles)
    sines = jnp.sin(angles)
    return (jnp.concatenate([cosines, cosines], -1), jnp.concatenate([sines, sines], -1))


def apply_rotary(values, cosine_lookup, sine_lookup):
    half_dim = values.shape[-1] // 2
    turned = jnp.concatenate([-values[..., half_dim:], values[..., :half_dim]], -1)
    return values * cosine_lookup + turned * sine_lookup


def rotate_back(values, cosine_lookup, sine_lookup):
    half_dim = values.shape[-1] // 2
    shifted = values * sine_lookup
    turned = jnp.concatenate([shifted[..., half_dim:], -shifted[..., :half_dim]], -1)
    return values * cosine_lookup + turned


def visible_mask(positions, doc_rows, begin_row, end_row):
    return (positions[None, :] <= positions[begin_row:end_row, None]) & (
        doc_rows[None, :] == doc_rows[begin_row:end_row, None]
    )


def block_scores(query_row_block, key_rows, positions, doc_rows, begin_row, end_row, score_scale):
    scores = (
        jnp.einsum(
            "qhgd,khd->hgqk",
            query_row_block[begin_row:end_row],
            key_rows,
            preferred_element_type=jnp.float32,
        )
        * score_scale
    )
    return jnp.where(visible_mask(positions, doc_rows, begin_row, end_row), scores, NEG_LARGE)


def attend_forward(item, score_scale):
    query_row_block, key_rows, value_row_block, positions, doc_rows = item
    sequence_length = query_row_block.shape[0]
    block_rows = min(512, sequence_length)
    outputs = []
    totals = []
    for begin_row in range(0, sequence_length, block_rows):
        end_row = begin_row + block_rows
        scores = block_scores(
            query_row_block, key_rows, positions, doc_rows, begin_row, end_row, score_scale
        )
        highest = jnp.max(scores, axis=-1, keepdims=True)
        exponents = jnp.exp(scores - highest)
        denominator = jnp.sum(exponents, axis=-1, keepdims=True)
        prob_low = (exponents / denominator).astype(jnp.bfloat16)
        outputs.append(
            jnp.einsum(
                "hgqk,khd->qhgd", prob_low, value_row_block, preferred_element_type=jnp.float32
            )
        )
        totals.append((highest + jnp.log(denominator))[..., 0])
    return (jnp.concatenate(outputs, 0), jnp.concatenate(totals, -1))


def attend_backward(item, score_scale):
    query_row_block, key_rows, value_row_block, out_grads, log_totals, positions, doc_rows = item
    sequence_length = query_row_block.shape[0]
    block_rows = min(512, sequence_length)
    key_sum = jnp.zeros(key_rows.shape, jnp.float32)
    value_sum = jnp.zeros(value_row_block.shape, jnp.float32)
    query_parts = []
    for begin_row in range(0, sequence_length, block_rows):
        end_row = begin_row + block_rows
        scores = block_scores(
            query_row_block, key_rows, positions, doc_rows, begin_row, end_row, score_scale
        )
        probs = jnp.exp(scores - log_totals[..., begin_row:end_row, None])
        prob_grad = jnp.einsum(
            "qhgd,khd->hgqk",
            out_grads[begin_row:end_row],
            value_row_block,
            preferred_element_type=jnp.float32,
        )
        score_grad = (
            probs * (prob_grad - jnp.sum(prob_grad * probs, axis=-1, keepdims=True)) * score_scale
        ).astype(jnp.bfloat16)
        query_parts.append(
            jnp.einsum("hgqk,khd->qhgd", score_grad, key_rows, preferred_element_type=jnp.float32)
        )
        key_sum = key_sum + jnp.einsum(
            "hgqk,qhgd->khd",
            score_grad,
            query_row_block[begin_row:end_row],
            preferred_element_type=jnp.float32,
        )
        value_sum = value_sum + jnp.einsum(
            "hgqk,qhgd->khd",
            probs.astype(jnp.bfloat16),
            out_grads[begin_row:end_row],
            preferred_element_type=jnp.float32,
        )
    return (jnp.concatenate(query_parts, 0), key_sum, value_sum)


def dense(left, right):
    return jnp.dot(left, right, preferred_element_type=jnp.float32)


def flips(count, bit):
    return [(index, index ^ bit) for index in range(count)]


def gather_tokens(own):
    count = lax.axis_size("seq")
    if count != 4:
        return lax.all_gather(own, "seq", axis=0, tiled=True)
    half = own.shape[0] // 2
    across = lax.ppermute(own, "seq", flips(4, 1))
    along = lax.ppermute(own, "seq", flips(4, 2))
    far_top = lax.ppermute(along[:half], "seq", flips(4, 1))
    far_bottom = lax.ppermute(across[half:], "seq", flips(4, 2))
    return jnp.concatenate([own, across, along, far_top, far_bottom], 0)


def scatter_tokens(part):
    count = lax.axis_size("seq")
    if count != 4:
        return lax.psum_scatter(
            part.astype(jnp.bfloat16), "seq", scatter_dimension=0, tiled=True
        ).astype(jnp.float32)
    rows = part.shape[0] // 8
    low = part.astype(jnp.bfloat16)
    own_top, own_bottom, across_top, across_bottom, along_top, along_bottom, far_top, far_bottom = (
        low[index * rows : (index + 1) * rows] for index in range(8)
    )

    def plus(left, right):
        return (left.astype(jnp.float32) + right.astype(jnp.float32)).astype(jnp.bfloat16)

    relay_top = lax.ppermute(far_top, "seq", flips(4, 1))
    relay_bottom = lax.ppermute(far_bottom, "seq", flips(4, 2))
    from_across_top = lax.ppermute(across_top, "seq", flips(4, 1))
    from_along_bottom = lax.ppermute(along_bottom, "seq", flips(4, 2))
    from_along_top = lax.ppermute(plus(along_top, relay_top), "seq", flips(4, 2))
    from_across_bottom = lax.ppermute(plus(across_bottom, relay_bottom), "seq", flips(4, 1))
    top = (
        own_top.astype(jnp.float32)
        + from_across_top.astype(jnp.float32)
        + from_along_top.astype(jnp.float32)
    )
    bottom = (
        own_bottom.astype(jnp.float32)
        + from_along_bottom.astype(jnp.float32)
        + from_across_bottom.astype(jnp.float32)
    )
    return jnp.concatenate([top, bottom], 0)


def sum_everywhere(value):
    for axis in ("seq", "fsdp"):
        count = lax.axis_size(axis)
        if count & (count - 1):
            value = lax.psum(value, axis)
            continue
        terms = [value] + [
            lax.ppermute(value, axis, flips(count, bit)) for bit in range(1, count)
        ]
        while len(terms) > 1:
            terms = [terms[at] + terms[at + 1] for at in range(0, len(terms), 2)]
        value = terms[0]
    return value


def gather_weight(shard):
    return lax.all_gather(shard, "fsdp", axis=0, tiled=True)


def scatter_weight(total):
    return lax.psum_scatter(
        total.astype(jnp.bfloat16), "fsdp", scatter_dimension=0, tiled=True
    ).astype(jnp.float32)


def times_transposed(left, right):
    return jnp.einsum("re,de->rd", left, right, preferred_element_type=jnp.float32)


def outer(left, right):
    return jnp.einsum("rd,rf->df", left, right, preferred_element_type=jnp.float32)


def shards(
    block_input,
    out_grad,
    query_proj,
    key_projection,
    value_projection,
    outgate_proj,
    output_proj,
    ffgate_proj,
    ffup_proj,
    ffdown_proj,
    attn_gain,
    ffn_gain,
    query_gain,
    key_gain,
    piece_order,
    doc_ids,
):
    seq_devices = lax.axis_size("seq")
    micro_count, seq_count, local_len, feature_dim = block_input.shape
    full_len = local_len * seq_devices
    piece_len = full_len // piece_order.shape[2]
    query_width = query_proj.shape[1]
    key_width = key_projection.shape[1]
    hidden_width = ffgate_proj.shape[1]
    query_heads = query_width // HEAD_SIZE
    kv_heads = key_width // HEAD_SIZE
    heads_per_group = query_heads // kv_heads
    score_scale = HEAD_SIZE ** (-0.5)
    cuts = [query_width, query_width + key_width, query_width + 2 * key_width]
    micros = range(micro_count)
    place = lax.axis_index("seq")
    owners = place ^ jnp.arange(seq_devices) if seq_devices == 4 else jnp.arange(seq_devices)

    inputs = [block_input[m, 0].astype(jnp.float32) for m in micros]
    scale_one = [rms_scale(x) for x in inputs]
    first_normalized = [x * s for x, s in zip(inputs, scale_one)]
    attn_rows = [gather_tokens((x * attn_gain).astype(jnp.bfloat16)) for x in first_normalized]
    qkvg_full = gather_weight(
        jnp.concatenate([query_proj, key_projection, value_projection, outgate_proj], 1)
    )
    output_full = gather_weight(output_proj.T)
    gate_up_full = gather_weight(jnp.concatenate([ffgate_proj, ffup_proj], 1))
    down_full = gather_weight(ffdown_proj.T)
    cot_rows = [gather_tokens(out_grad[m, 0]) for m in micros]

    kept = []
    middle, scale_two, normed_two, ffn_rows = [], [], [], []
    for m in micros:
        pre = dense(attn_rows[m], qkvg_full)
        query_pre, key_pre, value_pre, gate_pre = jnp.split(pre, cuts, axis=1)
        query_pre = query_pre.reshape(full_len, query_heads, HEAD_SIZE)
        key_pre = key_pre.reshape(full_len, kv_heads, HEAD_SIZE)
        value_low = value_pre.astype(jnp.bfloat16).reshape(full_len, kv_heads, HEAD_SIZE)
        stored = (
            piece_order[m, 0][:, None] * piece_len
            + jnp.arange(piece_len, dtype=jnp.int32)[None, :]
        ).reshape(seq_devices, local_len)
        positions = stored[owners].reshape(full_len)
        doc_rows = doc_ids[m, 0][positions]
        cosine_lookup, sine_lookup = rope_tables(positions, HEAD_SIZE)
        cosine_lookup = cosine_lookup[:, None, :]
        sine_lookup = sine_lookup[:, None, :]
        query_scale = rms_scale(query_pre)
        query_normed = query_pre * query_scale
        query_low = apply_rotary(query_normed * query_gain, cosine_lookup, sine_lookup).astype(
            jnp.bfloat16
        )
        key_scale = rms_scale(key_pre)
        key_normed = key_pre * key_scale
        key_low = apply_rotary(key_normed * key_gain, cosine_lookup, sine_lookup).astype(
            jnp.bfloat16
        )
        query_seq = query_low.reshape(full_len, kv_heads, heads_per_group, HEAD_SIZE)
        attn_out, log_totals = attend_forward(
            (query_seq, key_low, value_low, positions, doc_rows), score_scale
        )
        attn_out = attn_out.reshape(full_len, query_width)
        gate_sig = jax.nn.sigmoid(gate_pre)
        gated_low = (attn_out * gate_sig).astype(jnp.bfloat16)
        now = inputs[m] + scatter_tokens(times_transposed(gated_low, output_full))
        middle.append(now)
        scale_two.append(rms_scale(now))
        normed_two.append(now * scale_two[m])
        ffn_rows.append(gather_tokens((normed_two[m] * ffn_gain).astype(jnp.bfloat16)))
        kept.append(
            (
                query_seq,
                key_low,
                value_low,
                positions,
                doc_rows,
                cosine_lookup,
                sine_lookup,
                query_scale,
                query_normed,
                key_scale,
                key_normed,
                attn_out,
                log_totals,
                gate_sig,
                gated_low,
            )
        )

    hidden, gate_ffn, up_ffn = [], [], []
    for m in micros:
        gate_up = dense(ffn_rows[m], gate_up_full)
        gate_ffn.append(gate_up[:, :hidden_width])
        up_ffn.append(gate_up[:, hidden_width:])
        hidden.append((jax.nn.silu(gate_ffn[m]) * up_ffn[m]).astype(jnp.bfloat16))
    down_grad = scatter_weight(sum(outer(cot_rows[m], hidden[m]) for m in micros))
    outputs, gate_grad, up_grad, ffn_in_grad = [], [], [], []
    for m in micros:
        hidden_grad = dense(cot_rows[m], down_full)
        gate_sigm = jax.nn.sigmoid(gate_ffn[m])
        gate_grad.append(
            (
                hidden_grad * up_ffn[m] * gate_sigm * (1.0 + gate_ffn[m] * (1.0 - gate_sigm))
            ).astype(jnp.bfloat16)
        )
        up_grad.append((hidden_grad * (gate_ffn[m] * gate_sigm)).astype(jnp.bfloat16))
        part = times_transposed(gate_grad[m], gate_up_full[:, :hidden_width]) + times_transposed(
            up_grad[m], gate_up_full[:, hidden_width:]
        )
        ffn_in_grad.append(scatter_tokens(part))
    gate_w_grad = scatter_weight(sum(outer(ffn_rows[m], gate_grad[m]) for m in micros))
    up_w_grad = scatter_weight(sum(outer(ffn_rows[m], up_grad[m]) for m in micros))
    for m in micros:
        block_out = middle[m] + scatter_tokens(times_transposed(hidden[m], down_full))
        outputs.append(block_out.astype(jnp.bfloat16))

    middle_grad, branch_rows, ffn_gain_sum = [], [], 0.0
    for m in micros:
        middle_grad.append(
            out_grad[m, 0].astype(jnp.float32)
            + rms_back(ffn_in_grad[m], normed_two[m], scale_two[m], ffn_gain)
        )
        ffn_gain_sum = ffn_gain_sum + jnp.sum(ffn_in_grad[m] * normed_two[m], axis=0)
        branch_rows.append(gather_tokens(middle_grad[m].astype(jnp.bfloat16)))
    output_grad = scatter_weight(sum(outer(branch_rows[m], kept[m][-1]) for m in micros))

    query_gain_sum, key_gain_sum, attn_gain_sum = 0.0, 0.0, 0.0
    qkvg_sum = 0.0
    input_grads = []
    for m in micros:
        (
            query_seq,
            key_low,
            value_low,
            positions,
            doc_rows,
            cosine_lookup,
            sine_lookup,
            query_scale,
            query_normed,
            key_scale,
            key_normed,
            attn_out,
            log_totals,
            gate_sig,
            gated_low,
        ) = kept[m]
        gated_grad = dense(branch_rows[m], output_full)
        attn_out_grad = (gated_grad * gate_sig).astype(jnp.bfloat16)
        outgate_pre_grad = (gated_grad * attn_out * gate_sig * (1.0 - gate_sig)).astype(
            jnp.bfloat16
        )
        query_grad_raw, key_grad_raw, value_grad_raw = attend_backward(
            (
                query_seq,
                key_low,
                value_low,
                attn_out_grad.reshape(full_len, kv_heads, heads_per_group, HEAD_SIZE),
                log_totals,
                positions,
                doc_rows,
            ),
            score_scale,
        )
        query_turned = rotate_back(
            query_grad_raw.reshape(full_len, query_heads, HEAD_SIZE), cosine_lookup, sine_lookup
        )
        query_pre_grad = (
            rms_back(query_turned, query_normed, query_scale, query_gain)
            .astype(jnp.bfloat16)
            .reshape(full_len, query_width)
        )
        query_gain_sum = query_gain_sum + jnp.sum(query_turned * query_normed, axis=(0, 1))
        key_turned = rotate_back(key_grad_raw, cosine_lookup, sine_lookup)
        key_pre_grad = (
            rms_back(key_turned, key_normed, key_scale, key_gain)
            .astype(jnp.bfloat16)
            .reshape(full_len, key_width)
        )
        key_gain_sum = key_gain_sum + jnp.sum(key_turned * key_normed, axis=(0, 1))
        value_pre_grad = value_grad_raw.reshape(full_len, key_width).astype(jnp.bfloat16)
        pre_grad = jnp.concatenate(
            [query_pre_grad, key_pre_grad, value_pre_grad, outgate_pre_grad], 1
        )
        attn_in_grad = scatter_tokens(times_transposed(pre_grad, qkvg_full))
        qkvg_sum = qkvg_sum + outer(attn_rows[m], pre_grad)
        input_grads.append(
            (
                middle_grad[m]
                + rms_back(attn_in_grad, first_normalized[m], scale_one[m], attn_gain)
            ).astype(jnp.bfloat16)
        )
        attn_gain_sum = attn_gain_sum + jnp.sum(attn_in_grad * first_normalized[m], axis=0)
    query_w_grad, key_w_grad, value_w_grad, outgate_w_grad = jnp.split(
        scatter_weight(qkvg_sum), cuts, axis=1
    )
    gains = sum_everywhere(
        jnp.concatenate([attn_gain_sum, ffn_gain_sum, query_gain_sum, key_gain_sum])
    )
    return (
        jnp.stack(outputs)[:, None],
        jnp.stack(input_grads)[:, None],
        query_w_grad,
        key_w_grad,
        value_w_grad,
        outgate_w_grad,
        output_grad.T,
        gate_w_grad,
        up_w_grad,
        down_grad.T,
        gains[:feature_dim],
        gains[feature_dim : 2 * feature_dim],
        gains[2 * feature_dim : 2 * feature_dim + HEAD_SIZE],
        gains[2 * feature_dim + HEAD_SIZE :],
    )


def solution(mesh):
    return jax.shard_map(
        shards,
        mesh=mesh,
        in_specs=(
            P(None, "fsdp", "seq", None),
            P(None, "fsdp", "seq", None),
            P("fsdp", "seq"),
            P("fsdp", "seq"),
            P("fsdp", "seq"),
            P("fsdp", "seq"),
            P("seq", "fsdp"),
            P("fsdp", "seq"),
            P("fsdp", "seq"),
            P("seq", "fsdp"),
            P(),
            P(),
            P(),
            P(),
            P(None, "fsdp", None),
            P(None, "fsdp", None),
        ),
        out_specs=(
            P(None, "fsdp", "seq", None),
            P(None, "fsdp", "seq", None),
            P("fsdp", "seq"),
            P("fsdp", "seq"),
            P("fsdp", "seq"),
            P("fsdp", "seq"),
            P("seq", "fsdp"),
            P("fsdp", "seq"),
            P("fsdp", "seq"),
            P("seq", "fsdp"),
            P(),
            P(),
            P(),
            P(),
        ),
        check_vma=False,
    )
```

```python
import functools
import math

import jax
import jax.numpy as jnp
from jax import lax
from jax.experimental import pallas as pl
from jax.experimental.pallas import tpu as pltpu
from jax.sharding import PartitionSpec as P


HEAD_SIZE = 128


EPSILON = 1e-06
ROPE_BASE = 5000000.0


def rms_scale(values):
    return lax.rsqrt(jnp.mean(values * values, axis=-1, keepdims=True) + EPSILON)


def rms_back(grad_out, normed, scales, gain):
    scaled_grad = grad_out * gain
    return scales * (scaled_grad - normed * jnp.mean(scaled_grad * normed, axis=-1, keepdims=True))


def rope_tables(positions, head_dim):
    half_dim = head_dim // 2
    inverse = jnp.exp(
        -math.log(ROPE_BASE) * 2.0 * jnp.arange(half_dim, dtype=jnp.float32) / head_dim
    )
    angles = positions.astype(jnp.float32)[:, None] * inverse[None, :]
    cosines = jnp.cos(angles)
    sines = jnp.sin(angles)
    return (jnp.concatenate([cosines, cosines], -1), jnp.concatenate([sines, sines], -1))


def dense(left, right):
    return jnp.dot(left, right, preferred_element_type=jnp.float32)


def flips(count, bit):
    return [(index, index ^ bit) for index in range(count)]


def gather_tokens(own, relayed=True):
    count = lax.axis_size("seq")
    if count != 4:
        return lax.all_gather(own, "seq", axis=0, tiled=True)
    if not relayed:
        others = [lax.ppermute(own, "seq", flips(4, bit)) for bit in (1, 2, 3)]
        return jnp.concatenate([own] + others, 0)
    half = own.shape[0] // 2
    across = lax.ppermute(own, "seq", flips(4, 1))
    along = lax.ppermute(own, "seq", flips(4, 2))
    far_top, far_bottom = along[:half], across[half:]
    far_top = lax.ppermute(far_top, "seq", flips(4, 1))
    far_bottom = lax.ppermute(far_bottom, "seq", flips(4, 2))
    return jnp.concatenate([own, across, along, far_top, far_bottom], 0)


def scatter_tokens(part, relayed=False):
    count = lax.axis_size("seq")
    low = part.astype(jnp.bfloat16)
    if count != 4:
        return lax.psum_scatter(low, "seq", scatter_dimension=0, tiled=True).astype(jnp.float32)
    rows = part.shape[0] // 4
    own, across, along, far = (low[index * rows : (index + 1) * rows] for index in range(4))
    if not relayed:
        parts = [
            lax.ppermute(piece, "seq", flips(4, bit))
            for bit, piece in ((1, across), (2, along), (3, far))
        ]
        return sum((piece.astype(jnp.float32) for piece in parts), own.astype(jnp.float32))
    half = rows // 2
    relay_top = lax.ppermute(far[:half], "seq", flips(4, 1))
    relay_bottom = lax.ppermute(far[half:], "seq", flips(4, 2))

    def plus(left, right, before):
        right = jnp.pad(right.astype(jnp.float32), ((before, half - before), (0, 0)))
        return (left.astype(jnp.float32) + right).astype(jnp.bfloat16)

    to_across = plus(across, relay_bottom, half)
    to_along = plus(along, relay_top, 0)
    from_across = lax.ppermute(to_across, "seq", flips(4, 1))
    from_along = lax.ppermute(to_along, "seq", flips(4, 2))
    return (
        own.astype(jnp.float32) + from_across.astype(jnp.float32) + from_along.astype(jnp.float32)
    )


def sum_everywhere(value):
    for axis in ("seq", "fsdp"):
        count = lax.axis_size(axis)
        if count & (count - 1):
            value = lax.psum(value, axis)
            continue
        terms = [value] + [
            lax.ppermute(value, axis, flips(count, bit)) for bit in range(1, count)
        ]
        while len(terms) > 1:
            terms = [terms[at] + terms[at + 1] for at in range(0, len(terms), 2)]
        value = terms[0]
    return value


def gather_weight(shard):
    return lax.all_gather(shard, "fsdp", axis=0, tiled=True)


def scatter_weight(total):
    low = total.astype(jnp.bfloat16)
    low = lax.psum_scatter(low, "fsdp", scatter_dimension=0, tiled=True)
    return low.astype(jnp.float32)


def times_transposed(left, right):
    return jnp.einsum("re,de->rd", left, right, preferred_element_type=jnp.float32)


def rounded(value):
    return value.astype(jnp.bfloat16).astype(jnp.float32)


def outer_sum(lefts, rights):
    total = None
    for m in range(len(lefts)):
        part = outer(lefts[m], rights[m])
        total = part if total is None else part + rounded(total)
    return total


def outer(left, right):
    return jnp.einsum("rd,rf->df", left, right, preferred_element_type=jnp.float32)


def turn(values):
    return pltpu.roll(values, HEAD_SIZE // 2, 1)


def unit(values):
    scale = lax.rsqrt(jnp.mean(values * values, axis=-1, keepdims=True) + EPSILON)
    return values * scale, scale


def window_mask(doc_col_ref, doc_row_ref, begin, low, high):
    same = doc_col_ref[begin:high, :] == doc_row_ref[:, low:high]
    query_at = lax.broadcasted_iota(jnp.int32, same.shape, 0) + begin
    key_at = lax.broadcasted_iota(jnp.int32, same.shape, 1) + low
    return same & (key_at <= query_at)


def dot_last(left, right):
    return lax.dot_general(
        left, right, (((1,), (1,)), ((), ())), preferred_element_type=jnp.float32
    )


def dot_first(left, right):
    return lax.dot_general(
        left, right, (((0,), (0,)), ((), ())), preferred_element_type=jnp.float32
    )


def column(start, index, width):
    return pl.ds(pl.multiple_of(start + index * width, HEAD_SIZE), width)


def head_columns(kv_heads, group):
    at = pl.program_id(0)
    wide = group * HEAD_SIZE
    starts = [head * HEAD_SIZE for head in range(group)]
    keys = kv_heads * wide
    values = keys + kv_heads * HEAD_SIZE
    gates = values + kv_heads * HEAD_SIZE
    spots = [pl.ds(pl.multiple_of(start + at * wide, HEAD_SIZE), HEAD_SIZE) for start in starts]
    spots.append(column(keys, at, HEAD_SIZE))
    spots.append(column(values, at, HEAD_SIZE))
    spots.extend(
        pl.ds(pl.multiple_of(gates + start + at * wide, HEAD_SIZE), HEAD_SIZE) for start in starts
    )
    return spots


def load_heads(
    spots, slots, pre_ref, cos_ref, sin_ref, query_gain_ref, key_gain_ref, q_s, k_s, v_s, tile, group
):
    for at in range(pre_ref.shape[0] // tile):
        rows = pl.ds(pl.multiple_of(slots[at] * tile, tile), tile)
        here = slice(at * tile, (at + 1) * tile)
        cosine, sine = cos_ref[here, :], sin_ref[here, :]
        for head in range(group + 1):
            normed, _ = unit(pre_ref[rows, spots[head]])
            scaled = normed * (query_gain_ref if head < group else key_gain_ref)[...]
            turned = (scaled * cosine + turn(scaled) * sine).astype(jnp.bfloat16)
            if head < group:
                q_s[here, head * HEAD_SIZE : (head + 1) * HEAD_SIZE] = turned
            else:
                k_s[here, :] = turned
        v_s[here, :] = pre_ref[rows, spots[group + 1]].astype(jnp.bfloat16)


def forward_kernel(
    slots,
    pre_ref,
    cos_ref,
    sin_ref,
    doc_col_ref,
    doc_row_ref,
    query_gain_ref,
    key_gain_ref,
    gated_ref,
    attn_ref,
    prob_ref,
    q_s,
    k_s,
    v_s,
    *,
    tile,
    window,
    kv_heads,
    group,
):
    spots = head_columns(kv_heads, group)
    factor = HEAD_SIZE ** (-0.5) * math.log2(math.e)
    load_heads(
        spots, slots, pre_ref, cos_ref, sin_ref, query_gain_ref, key_gain_ref, q_s, k_s, v_s, tile, group
    )
    for at in range(pre_ref.shape[0] // tile):
        begin, high = at * tile, (at + 1) * tile
        low = max(0, at - window) * tile
        mask = window_mask(doc_col_ref, doc_row_ref, begin, low, high)
        rows = pl.ds(pl.multiple_of(slots[at] * tile, tile), tile)
        for head in range(group):
            cut = slice(head * HEAD_SIZE, (head + 1) * HEAD_SIZE)
            scores = dot_last(q_s[begin:high, cut], k_s[low:high, :])
            weights = jnp.where(mask, jnp.exp2(scores * factor), 0.0)
            total = jnp.sum(weights, axis=-1, keepdims=True)
            probs = (weights * (1.0 / total)).astype(jnp.bfloat16)
            prob_ref[head, begin:high, : high - low] = probs
            out = jnp.dot(probs, v_s[low:high, :], preferred_element_type=jnp.float32)
            gate_pre = pre_ref[rows, spots[group + 2 + head]]
            gated_ref[rows, cut] = (out * jax.nn.sigmoid(gate_pre)).astype(jnp.bfloat16)
            attn_ref[begin:high, cut] = out


def backward_kernel(
    slots,
    pre_ref,
    grad_ref,
    attn_ref,
    prob_ref,
    q_ref,
    k_ref,
    v_ref,
    cos_ref,
    sin_ref,
    query_gain_ref,
    key_gain_ref,
    out_ref,
    query_sum_ref,
    key_sum_ref,
    dk_s,
    dv_s,
    *,
    tile,
    window,
    kv_heads,
    group,
):
    spots = head_columns(kv_heads, group)
    score_scale = HEAD_SIZE ** (-0.5)
    count = pre_ref.shape[0] // tile
    dk_s[...] = jnp.zeros_like(dk_s)
    dv_s[...] = jnp.zeros_like(dv_s)

    def back(turned_grad, at, rows, head, gain):
        here = slice(at * tile, (at + 1) * tile)
        straight = turned_grad * cos_ref[here, :] - turn(turned_grad) * sin_ref[here, :]
        normed, scale = unit(pre_ref[rows, spots[head]])
        scaled = straight * gain
        shared = jnp.mean(scaled * normed, axis=-1, keepdims=True)
        out_ref[rows, spots[head]] = (
            scale * (scaled - normed * shared)
        ).astype(jnp.bfloat16)
        return jnp.sum(straight * normed, axis=0, keepdims=True)

    query_sum = jnp.zeros((1, HEAD_SIZE), jnp.float32)
    for at in range(count):
        begin, high = at * tile, (at + 1) * tile
        low = max(0, at - window) * tile
        rows = pl.ds(pl.multiple_of(slots[at] * tile, tile), tile)
        for head in range(group):
            cut = slice(head * HEAD_SIZE, (head + 1) * HEAD_SIZE)
            gate_sig = jax.nn.sigmoid(pre_ref[rows, spots[group + 2 + head]])
            gated_grad = grad_ref[rows, cut]
            attn_out = attn_ref[begin:high, cut]
            out_low = (gated_grad * gate_sig).astype(jnp.bfloat16)
            out_ref[rows, spots[group + 2 + head]] = (
                gated_grad * attn_out * gate_sig * (1.0 - gate_sig)
            ).astype(jnp.bfloat16)
            delta = jnp.sum(out_low.astype(jnp.float32) * attn_out, axis=-1, keepdims=True)
            probs = prob_ref[head, begin:high, : high - low]
            prob_grad = dot_last(out_low, v_ref[low:high, :])
            score_grad = (probs.astype(jnp.float32) * (prob_grad - delta)).astype(jnp.bfloat16)
            query_grad = jnp.dot(
                score_grad, k_ref[low:high, :], preferred_element_type=jnp.float32
            )
            dk_s[low:high, :] += dot_first(score_grad, q_ref[begin:high, cut])
            dv_s[low:high, :] += dot_first(probs, out_low)
            query_sum = query_sum + back(
                query_grad * score_scale, at, rows, head, query_gain_ref[...]
            )
    query_sum_ref[0] = query_sum
    key_sum = jnp.zeros((1, HEAD_SIZE), jnp.float32)
    for at in range(count):
        here = slice(at * tile, (at + 1) * tile)
        rows = pl.ds(pl.multiple_of(slots[at] * tile, tile), tile)
        key_sum = key_sum + back(
            dk_s[here, :] * score_scale, at, rows, group, key_gain_ref[...]
        )
        out_ref[rows, spots[group + 1]] = dv_s[
            here, :
        ].astype(jnp.bfloat16)
    key_sum_ref[0] = key_sum


def whole_block(shape):
    return pl.BlockSpec(shape, lambda head, slots: (0,) * len(shape))


def head_block(rows, width):
    return pl.BlockSpec((rows, width), lambda head, slots: (0, head))


def attention_forward(slots, pre, tables, tile, window, kv_heads, group):
    rows, width = pre.shape
    heads = group * HEAD_SIZE
    span = (window + 1) * tile
    pairs = kv_heads * group * rows * span
    return pl.pallas_call(
        functools.partial(
            forward_kernel, tile=tile, window=window, kv_heads=kv_heads, group=group
        ),
        grid_spec=pltpu.PrefetchScalarGridSpec(
            num_scalar_prefetch=1,
            grid=(kv_heads,),
            in_specs=[
                whole_block((rows, width)),
                whole_block((rows, HEAD_SIZE)),
                whole_block((rows, HEAD_SIZE)),
                whole_block((rows, 1)),
                whole_block((1, rows)),
                whole_block((1, HEAD_SIZE)),
                whole_block((1, HEAD_SIZE)),
            ],
            out_specs=[
                head_block(rows, heads),
                head_block(rows, heads),
                pl.BlockSpec((group, rows, span), lambda head, slots: (head, 0, 0)),
                head_block(rows, heads),
                head_block(rows, HEAD_SIZE),
                head_block(rows, HEAD_SIZE),
            ],
        ),
        out_shape=[
            jax.ShapeDtypeStruct((rows, kv_heads * heads), jnp.bfloat16),
            jax.ShapeDtypeStruct((rows, kv_heads * heads), jnp.float32),
            jax.ShapeDtypeStruct((kv_heads * group, rows, span), jnp.bfloat16),
            jax.ShapeDtypeStruct((rows, kv_heads * heads), jnp.bfloat16),
            jax.ShapeDtypeStruct((rows, kv_heads * HEAD_SIZE), jnp.bfloat16),
            jax.ShapeDtypeStruct((rows, kv_heads * HEAD_SIZE), jnp.bfloat16),
        ],
        cost_estimate=pl.CostEstimate(
            flops=20 * pairs * HEAD_SIZE, bytes_accessed=rows * width * 8, transcendentals=pairs
        ),
        name="attend_fwd",
    )(slots, pre, *tables)


def attention_backward(
    slots, pre, gated_grad, saved, cos, sin, gains, tile, window, kv_heads, group
):
    rows, width = pre.shape
    heads = group * HEAD_SIZE
    span = (window + 1) * tile
    pairs = kv_heads * group * rows * span
    return pl.pallas_call(
        functools.partial(
            backward_kernel, tile=tile, window=window, kv_heads=kv_heads, group=group
        ),
        grid_spec=pltpu.PrefetchScalarGridSpec(
            num_scalar_prefetch=1,
            grid=(kv_heads,),
            in_specs=[
                whole_block((rows, width)),
                head_block(rows, heads),
                head_block(rows, heads),
                pl.BlockSpec((group, rows, span), lambda head, slots: (head, 0, 0)),
                head_block(rows, heads),
                head_block(rows, HEAD_SIZE),
                head_block(rows, HEAD_SIZE),
                whole_block((rows, HEAD_SIZE)),
                whole_block((rows, HEAD_SIZE)),
                whole_block((1, HEAD_SIZE)),
                whole_block((1, HEAD_SIZE)),
            ],
            out_specs=[whole_block((rows, width))]
            + [pl.BlockSpec((1, 1, HEAD_SIZE), lambda head, slots: (head, 0, 0))] * 2,
            scratch_shapes=[
                pltpu.VMEM((rows, HEAD_SIZE), jnp.float32),
                pltpu.VMEM((rows, HEAD_SIZE), jnp.float32),
            ],
        ),
        out_shape=[
            jax.ShapeDtypeStruct((rows, width), jnp.bfloat16),
            jax.ShapeDtypeStruct((kv_heads, 1, HEAD_SIZE), jnp.float32),
            jax.ShapeDtypeStruct((kv_heads, 1, HEAD_SIZE), jnp.float32),
        ],
        cost_estimate=pl.CostEstimate(
            flops=40 * pairs * HEAD_SIZE, bytes_accessed=rows * width * 16, transcendentals=pairs
        ),
        name="attend_bwd",
    )(slots, pre, gated_grad, *saved, cos, sin, *gains)


def shards(
    block_input,
    out_grad,
    query_proj,
    key_projection,
    value_projection,
    outgate_proj,
    output_proj,
    ffgate_proj,
    ffup_proj,
    ffdown_proj,
    attn_gain,
    ffn_gain,
    query_gain,
    key_gain,
    piece_order,
    doc_ids,
):
    seq_devices = lax.axis_size("seq")
    micro_count, _, local_len, feature_dim = block_input.shape
    full_len = local_len * seq_devices
    piece_len = full_len // piece_order.shape[2]
    query_width = query_proj.shape[1]
    key_width = key_projection.shape[1]
    hidden_width = ffgate_proj.shape[1]
    query_heads = query_width // HEAD_SIZE
    kv_heads = key_width // HEAD_SIZE
    heads_per_group = query_heads // kv_heads
    window = -(-(full_len // 2 - 1) // piece_len)
    micros = range(micro_count)
    place = lax.axis_index("seq")
    chunk = local_len // piece_len
    owners = place ^ jnp.arange(seq_devices) if seq_devices == 4 else jnp.arange(seq_devices)

    attn_gains, ffn_gains, documents = zip(
        *(lax.optimization_barrier((attn_gain, ffn_gain, doc_ids[m, 0])) for m in micros)
    )
    inputs = [block_input[m, 0].astype(jnp.float32) for m in micros]
    scale_one = [rms_scale(x) for x in inputs]
    first_normalized = [x * s for x, s in zip(inputs, scale_one)]
    attn_rows = [
        gather_tokens((x * attn_gains[m]).astype(jnp.bfloat16))
        for m, x in enumerate(first_normalized)
    ]
    qkvg_full = gather_weight(
        jnp.concatenate([query_proj, key_projection, value_projection, outgate_proj], 1)
    )
    output_full = gather_weight(output_proj.T)
    gate_up_full = gather_weight(jnp.concatenate([ffgate_proj, ffup_proj], 1))
    down_full = gather_weight(ffdown_proj.T)
    cot_rows = [gather_tokens(out_grad[m, 0], relayed=m == 0) for m in micros]

    cosines, sines = rope_tables(jnp.arange(full_len, dtype=jnp.int32), HEAD_SIZE)
    sines = sines * jnp.where(jnp.arange(HEAD_SIZE) < HEAD_SIZE // 2, -1.0, 1.0)
    attention = dict(tile=piece_len, window=window, kv_heads=kv_heads, group=heads_per_group)
    kept = []
    middle, scale_two, normed_two, ffn_rows = [], [], [], []
    for m in micros:
        pre = dense(attn_rows[m], qkvg_full)
        held = piece_order[m, 0].reshape(seq_devices, chunk)[owners].reshape(-1)
        at = jnp.arange(held.shape[0], dtype=jnp.int32)
        slots = jnp.sum(jnp.where(held[None, :] == at[:, None], at[None, :], 0), axis=1)
        tables = (
            cosines,
            sines,
            documents[m][:, None],
            documents[m][None, :],
            query_gain[None, :],
            key_gain[None, :],
        )
        gated_low, *saved = attention_forward(slots, pre, tables, **attention)
        part = times_transposed(gated_low, output_full)
        branch = scatter_tokens(part, relayed=True)
        held = (block_input, branch) + tuple(normed_two[-1:])
        held, branch = lax.optimization_barrier(held)[:2]
        now = held[m, 0].astype(jnp.float32) + branch
        middle.append(now)
        scale_two.append(rms_scale(now))
        normed_two.append(now * scale_two[m])
        ffn_rows.append(gather_tokens((normed_two[m] * ffn_gains[m]).astype(jnp.bfloat16)))
        kept.append((slots, pre, saved, tables, gated_low))

    hidden, gate_ffn, up_ffn = [], [], []
    for m in micros:
        gate_up = dense(ffn_rows[m], gate_up_full)
        low = (jax.nn.silu(gate_up[:, :hidden_width]) * gate_up[:, hidden_width:]).astype(
            jnp.bfloat16
        )
        low, gate_up = lax.optimization_barrier((low, gate_up))
        hidden.append(low)
        gate_ffn.append(gate_up[:, :hidden_width])
        up_ffn.append(gate_up[:, hidden_width:])
    down_grad = scatter_weight(outer_sum(cot_rows, hidden))
    outputs, gate_grad, up_grad, ffn_in_grad = [], [], [], []
    for m in micros:
        hidden_grad = dense(cot_rows[m], down_full)
        gate_sigm = jax.nn.sigmoid(gate_ffn[m])
        gate_grad.append(
            (
                hidden_grad * up_ffn[m] * gate_sigm * (1.0 + gate_ffn[m] * (1.0 - gate_sigm))
            ).astype(jnp.bfloat16)
        )
        up_grad.append((hidden_grad * (gate_ffn[m] * gate_sigm)).astype(jnp.bfloat16))
        part = times_transposed(up_grad[m], gate_up_full[:, hidden_width:])
        part = times_transposed(gate_grad[m], gate_up_full[:, :hidden_width]) + rounded(part)
        ffn_in_grad.append(scatter_tokens(part, relayed=True))
    gate_w_grad = scatter_weight(outer_sum(ffn_rows, gate_grad))
    up_w_grad = scatter_weight(outer_sum(ffn_rows, up_grad))
    middle_grad, branch_rows, ffn_gain_sum = [], [], 0.0
    for m in micros:
        held = (out_grad, ffn_in_grad[m]) + tuple(middle_grad[-1:])
        held, ffn_in_grad[m] = lax.optimization_barrier(held)[:2]
        middle_grad.append(
            held[m, 0].astype(jnp.float32)
            + rms_back(ffn_in_grad[m], normed_two[m], scale_two[m], ffn_gains[m])
        )
        middle_grad[m], middle[m] = lax.optimization_barrier((middle_grad[m], middle[m]))
        ffn_gain_sum = ffn_gain_sum + jnp.sum(ffn_in_grad[m] * normed_two[m], axis=0)
        branch_rows.append(gather_tokens(middle_grad[m].astype(jnp.bfloat16)))
    for m in micros:
        part = times_transposed(hidden[m], down_full)
        outputs.append((middle[m] + scatter_tokens(part, relayed=True)).astype(jnp.bfloat16))
    output_grad = scatter_weight(outer_sum(branch_rows, [held[-1] for held in kept]))

    query_gain_sum, key_gain_sum, attn_gain_sum = 0.0, 0.0, 0.0
    pre_grads = []
    input_grads = []
    for m in micros:
        slots, pre, saved, tables, gated_low = kept[m]
        gated_grad = dense(branch_rows[m], output_full)
        pre_grad, query_sums, key_sums = attention_backward(
            slots, pre, gated_grad, saved, *tables[:2], tables[-2:], **attention
        )
        query_gain_sum = query_gain_sum + jnp.sum(query_sums, axis=(0, 1))
        key_gain_sum = key_gain_sum + jnp.sum(key_sums, axis=(0, 1))
        attn_in_grad = scatter_tokens(times_transposed(pre_grad, qkvg_full), relayed=True)
        held = (block_input, attn_in_grad) + tuple(input_grads[-1:])
        held, attn_in_grad = lax.optimization_barrier(held)[:2]
        back_normed = held[m, 0].astype(jnp.float32) * scale_one[m]
        pre_grads.append(pre_grad)
        input_grads.append(
            (
                middle_grad[m]
                + rms_back(attn_in_grad, back_normed, scale_one[m], attn_gains[m])
            ).astype(jnp.bfloat16)
        )
        attn_gain_sum = attn_gain_sum + jnp.sum(attn_in_grad * back_normed, axis=0)
    qkvg_grad = scatter_weight(outer_sum(attn_rows, pre_grads))
    cuts = [query_width, query_width + key_width, query_width + 2 * key_width]
    query_w_grad, key_w_grad, value_w_grad, outgate_w_grad = jnp.split(qkvg_grad, cuts, axis=1)
    gains = sum_everywhere(
        jnp.concatenate([attn_gain_sum, ffn_gain_sum, query_gain_sum, key_gain_sum])
    )
    return (
        jnp.stack(outputs)[:, None],
        jnp.stack(input_grads)[:, None],
        query_w_grad,
        key_w_grad,
        value_w_grad,
        outgate_w_grad,
        output_grad.T,
        gate_w_grad,
        up_w_grad,
        down_grad.T,
        gains[:feature_dim],
        gains[feature_dim : 2 * feature_dim],
        gains[2 * feature_dim : 2 * feature_dim + HEAD_SIZE],
        gains[2 * feature_dim + HEAD_SIZE :],
    )


def solution(mesh):
    return jax.shard_map(
        shards,
        mesh=mesh,
        in_specs=(
            P(None, "fsdp", "seq", None),
            P(None, "fsdp", "seq", None),
            P("fsdp", "seq"),
            P("fsdp", "seq"),
            P("fsdp", "seq"),
            P("fsdp", "seq"),
            P("seq", "fsdp"),
            P("fsdp", "seq"),
            P("fsdp", "seq"),
            P("seq", "fsdp"),
            P(),
            P(),
            P(),
            P(),
            P(None, "fsdp", None),
            P(None, "fsdp", None),
        ),
        out_specs=(
            P(None, "fsdp", "seq", None),
            P(None, "fsdp", "seq", None),
            P("fsdp", "seq"),
            P("fsdp", "seq"),
            P("fsdp", "seq"),
            P("fsdp", "seq"),
            P("seq", "fsdp"),
            P("fsdp", "seq"),
            P("fsdp", "seq"),
            P("seq", "fsdp"),
            P(),
            P(),
            P(),
            P(),
        ),
        check_vma=False,
    )
```

```python
import functools
import math

import jax
import jax.numpy as jnp
from jax import lax
from jax.experimental import pallas as pl
from jax.experimental.pallas import tpu as pltpu
from jax.sharding import PartitionSpec as P


HEAD_SIZE = 128


EPSILON = 1e-06
ROPE_BASE = 5000000.0


def rms_scale(values):
    return lax.rsqrt(jnp.mean(values * values, axis=-1, keepdims=True) + EPSILON)


def rms_back(grad_out, normed, scales, gain):
    scaled_grad = grad_out * gain
    return scales * (scaled_grad - normed * jnp.mean(scaled_grad * normed, axis=-1, keepdims=True))


def rope_tables(positions, head_dim):
    half_dim = head_dim // 2
    inverse = jnp.exp(
        -math.log(ROPE_BASE) * 2.0 * jnp.arange(half_dim, dtype=jnp.float32) / head_dim
    )
    angles = positions.astype(jnp.float32)[:, None] * inverse[None, :]
    cosines = jnp.cos(angles)
    sines = jnp.sin(angles)
    return (jnp.concatenate([cosines, cosines], -1), jnp.concatenate([sines, sines], -1))


def dense(left, right):
    return jnp.dot(left, right, preferred_element_type=jnp.float32)


def flips(count, bit):
    return [(index, index ^ bit) for index in range(count)]


def gather_tokens(own, relayed=True):
    count = lax.axis_size("seq")
    if count != 4:
        return lax.all_gather(own, "seq", axis=0, tiled=True)
    if not relayed:
        others = [lax.ppermute(own, "seq", flips(4, bit)) for bit in (1, 2, 3)]
        return jnp.concatenate([own] + others, 0)
    half = own.shape[0] // 2
    across = lax.ppermute(own, "seq", flips(4, 1))
    along = lax.ppermute(own, "seq", flips(4, 2))
    far_top, far_bottom = along[:half], across[half:]
    far_top = lax.ppermute(far_top, "seq", flips(4, 1))
    far_bottom = lax.ppermute(far_bottom, "seq", flips(4, 2))
    return jnp.concatenate([own, across, along, far_top, far_bottom], 0)


def scatter_tokens(part, relayed=False):
    count = lax.axis_size("seq")
    low = part.astype(jnp.bfloat16)
    if count != 4:
        return lax.psum_scatter(low, "seq", scatter_dimension=0, tiled=True).astype(jnp.float32)
    rows = part.shape[0] // 4
    own, across, along, far = (low[index * rows : (index + 1) * rows] for index in range(4))
    if not relayed:
        parts = [
            lax.ppermute(piece, "seq", flips(4, bit))
            for bit, piece in ((1, across), (2, along), (3, far))
        ]
        return sum((piece.astype(jnp.float32) for piece in parts), own.astype(jnp.float32))
    half = rows // 2
    relay_top = lax.ppermute(far[:half], "seq", flips(4, 1))
    relay_bottom = lax.ppermute(far[half:], "seq", flips(4, 2))

    def plus(left, right, before):
        right = jnp.pad(right.astype(jnp.float32), ((before, half - before), (0, 0)))
        return (left.astype(jnp.float32) + right).astype(jnp.bfloat16)

    to_across = plus(across, relay_bottom, half)
    to_along = plus(along, relay_top, 0)
    from_across = lax.ppermute(to_across, "seq", flips(4, 1))
    from_along = lax.ppermute(to_along, "seq", flips(4, 2))
    return (
        own.astype(jnp.float32) + from_across.astype(jnp.float32) + from_along.astype(jnp.float32)
    )


def sum_everywhere(value):
    for axis in ("seq", "fsdp"):
        count = lax.axis_size(axis)
        if count & (count - 1):
            value = lax.psum(value, axis)
            continue
        terms = [value] + [lax.ppermute(value, axis, flips(count, bit)) for bit in range(1, count)]
        while len(terms) > 1:
            terms = [terms[at] + terms[at + 1] for at in range(0, len(terms), 2)]
        value = terms[0]
    return value


def gather_weight(shard):
    return lax.all_gather(shard, "fsdp", axis=0, tiled=True)


def scatter_weight(total):
    low = total.astype(jnp.bfloat16)
    low = lax.psum_scatter(low, "fsdp", scatter_dimension=0, tiled=True)
    return low.astype(jnp.float32)


def times_transposed(left, right):
    return jnp.einsum("re,de->rd", left, right, preferred_element_type=jnp.float32)


def rounded(value):
    return value.astype(jnp.bfloat16).astype(jnp.float32)


def outer_sum(lefts, rights):
    total = None
    for m in range(len(lefts)):
        part = outer(lefts[m], rights[m])
        total = part if total is None else part + rounded(total)
    return total


def outer(left, right):
    return jnp.einsum("rd,rf->df", left, right, preferred_element_type=jnp.float32)


def turn(values):
    return pltpu.roll(values, HEAD_SIZE // 2, 1)


def unit(values):
    scale = lax.rsqrt(jnp.mean(values * values, axis=-1, keepdims=True) + EPSILON)
    return values * scale, scale


def window_mask(doc_col_ref, doc_row_ref, begin, low, high):
    same = doc_col_ref[begin:high, :] == doc_row_ref[:, low:high]
    query_at = lax.broadcasted_iota(jnp.int32, same.shape, 0) + begin
    key_at = lax.broadcasted_iota(jnp.int32, same.shape, 1) + low
    return same & (key_at <= query_at)


def dot_last(left, right):
    return lax.dot_general(
        left, right, (((1,), (1,)), ((), ())), preferred_element_type=jnp.float32
    )


def dot_first(left, right):
    return lax.dot_general(
        left, right, (((0,), (0,)), ((), ())), preferred_element_type=jnp.float32
    )


def column(start, index, width):
    return pl.ds(pl.multiple_of(start + index * width, HEAD_SIZE), width)


def head_columns(kv_heads, group):
    at = pl.program_id(0)
    wide = group * HEAD_SIZE
    starts = [head * HEAD_SIZE for head in range(group)]
    keys = kv_heads * wide
    values = keys + kv_heads * HEAD_SIZE
    gates = values + kv_heads * HEAD_SIZE
    spots = [pl.ds(pl.multiple_of(start + at * wide, HEAD_SIZE), HEAD_SIZE) for start in starts]
    spots.append(column(keys, at, HEAD_SIZE))
    spots.append(column(values, at, HEAD_SIZE))
    spots.extend(
        pl.ds(pl.multiple_of(gates + start + at * wide, HEAD_SIZE), HEAD_SIZE) for start in starts
    )
    return spots


def load_heads(
    spots, slots, pre_ref, cos_ref, sin_ref, query_gain_ref, key_gain_ref, q_s, k_s, v_s, tile, group
):
    for at in range(pre_ref.shape[0] // tile):
        rows = pl.ds(pl.multiple_of(slots[at] * tile, tile), tile)
        here = slice(at * tile, (at + 1) * tile)
        cosine, sine = cos_ref[here, :], sin_ref[here, :]
        for head in range(group + 1):
            normed, _ = unit(pre_ref[rows, spots[head]])
            scaled = normed * (query_gain_ref if head < group else key_gain_ref)[...]
            turned = (scaled * cosine + turn(scaled) * sine).astype(jnp.bfloat16)
            if head < group:
                q_s[here, head * HEAD_SIZE : (head + 1) * HEAD_SIZE] = turned
            else:
                k_s[here, :] = turned
        v_s[here, :] = pre_ref[rows, spots[group + 1]].astype(jnp.bfloat16)


def forward_kernel(
    slots,
    pre_ref,
    cos_ref,
    sin_ref,
    doc_col_ref,
    doc_row_ref,
    query_gain_ref,
    key_gain_ref,
    gated_ref,
    attn_ref,
    prob_ref,
    q_s,
    k_s,
    v_s,
    *,
    tile,
    window,
    kv_heads,
    group,
):
    spots = head_columns(kv_heads, group)
    factor = HEAD_SIZE ** (-0.5) * math.log2(math.e)
    load_heads(
        spots, slots, pre_ref, cos_ref, sin_ref, query_gain_ref, key_gain_ref, q_s, k_s, v_s, tile, group
    )
    for at in range(pre_ref.shape[0] // tile):
        begin, high = at * tile, (at + 1) * tile
        low = max(0, at - window) * tile
        mask = window_mask(doc_col_ref, doc_row_ref, begin, low, high)
        rows = pl.ds(pl.multiple_of(slots[at] * tile, tile), tile)
        for head in range(group):
            cut = slice(head * HEAD_SIZE, (head + 1) * HEAD_SIZE)
            scores = dot_last(q_s[begin:high, cut], k_s[low:high, :])
            weights = jnp.where(mask, jnp.exp2(scores * factor), 0.0)
            total = jnp.sum(weights, axis=-1, keepdims=True)
            probs = (weights * (1.0 / total)).astype(jnp.bfloat16)
            prob_ref[head, begin:high, : high - low] = probs
            out = jnp.dot(probs, v_s[low:high, :], preferred_element_type=jnp.float32)
            gate_pre = pre_ref[rows, spots[group + 2 + head]]
            gated_ref[rows, cut] = (out * jax.nn.sigmoid(gate_pre)).astype(jnp.bfloat16)
            attn_ref[begin:high, cut] = out


def backward_kernel(
    slots,
    pre_ref,
    grad_ref,
    attn_ref,
    prob_ref,
    q_ref,
    k_ref,
    v_ref,
    cos_ref,
    sin_ref,
    query_gain_ref,
    key_gain_ref,
    out_ref,
    query_sum_ref,
    key_sum_ref,
    dk_s,
    dv_s,
    *,
    tile,
    window,
    kv_heads,
    group,
):
    spots = head_columns(kv_heads, group)
    score_scale = HEAD_SIZE ** (-0.5)
    count = pre_ref.shape[0] // tile
    dk_s[...] = jnp.zeros_like(dk_s)
    dv_s[...] = jnp.zeros_like(dv_s)

    def back(turned_grad, at, rows, head, gain):
        here = slice(at * tile, (at + 1) * tile)
        straight = turned_grad * cos_ref[here, :] - turn(turned_grad) * sin_ref[here, :]
        normed, scale = unit(pre_ref[rows, spots[head]])
        scaled = straight * gain
        shared = jnp.mean(scaled * normed, axis=-1, keepdims=True)
        out_ref[rows, spots[head]] = (
            scale * (scaled - normed * shared)
        ).astype(jnp.bfloat16)
        return jnp.sum(straight * normed, axis=0, keepdims=True)

    query_sum = jnp.zeros((1, HEAD_SIZE), jnp.float32)
    for at in range(count):
        begin, high = at * tile, (at + 1) * tile
        low = max(0, at - window) * tile
        rows = pl.ds(pl.multiple_of(slots[at] * tile, tile), tile)
        for head in range(group):
            cut = slice(head * HEAD_SIZE, (head + 1) * HEAD_SIZE)
            gate_sig = jax.nn.sigmoid(pre_ref[rows, spots[group + 2 + head]])
            gated_grad = grad_ref[rows, cut]
            attn_out = attn_ref[begin:high, cut]
            out_low = (gated_grad * gate_sig).astype(jnp.bfloat16)
            out_ref[rows, spots[group + 2 + head]] = (
                gated_grad * attn_out * gate_sig * (1.0 - gate_sig)
            ).astype(jnp.bfloat16)
            delta = jnp.sum(out_low.astype(jnp.float32) * attn_out, axis=-1, keepdims=True)
            probs = prob_ref[head, begin:high, : high - low]
            prob_grad = dot_last(out_low, v_ref[low:high, :])
            score_grad = (probs.astype(jnp.float32) * (prob_grad - delta)).astype(jnp.bfloat16)
            query_grad = jnp.dot(
                score_grad, k_ref[low:high, :], preferred_element_type=jnp.float32
            )
            dk_s[low:high, :] += dot_first(score_grad, q_ref[begin:high, cut])
            dv_s[low:high, :] += dot_first(probs, out_low)
            query_sum = query_sum + back(
                query_grad * score_scale, at, rows, head, query_gain_ref[...]
            )
    query_sum_ref[0] = query_sum
    key_sum = jnp.zeros((1, HEAD_SIZE), jnp.float32)
    for at in range(count):
        here = slice(at * tile, (at + 1) * tile)
        rows = pl.ds(pl.multiple_of(slots[at] * tile, tile), tile)
        key_sum = key_sum + back(
            dk_s[here, :] * score_scale, at, rows, group, key_gain_ref[...]
        )
        out_ref[rows, spots[group + 1]] = dv_s[
            here, :
        ].astype(jnp.bfloat16)
    key_sum_ref[0] = key_sum


def whole_block(shape):
    return pl.BlockSpec(shape, lambda head, slots: (0,) * len(shape))


def head_block(rows, width):
    return pl.BlockSpec((rows, width), lambda head, slots: (0, head))


def attention_forward(slots, pre, tables, tile, window, kv_heads, group):
    rows, width = pre.shape
    heads = group * HEAD_SIZE
    span = (window + 1) * tile
    pairs = kv_heads * group * rows * span
    return pl.pallas_call(
        functools.partial(
            forward_kernel, tile=tile, window=window, kv_heads=kv_heads, group=group
        ),
        grid_spec=pltpu.PrefetchScalarGridSpec(
            num_scalar_prefetch=1,
            grid=(kv_heads,),
            in_specs=[
                whole_block((rows, width)),
                whole_block((rows, HEAD_SIZE)),
                whole_block((rows, HEAD_SIZE)),
                whole_block((rows, 1)),
                whole_block((1, rows)),
                whole_block((1, HEAD_SIZE)),
                whole_block((1, HEAD_SIZE)),
            ],
            out_specs=[
                head_block(rows, heads),
                head_block(rows, heads),
                pl.BlockSpec((group, rows, span), lambda head, slots: (head, 0, 0)),
                head_block(rows, heads),
                head_block(rows, HEAD_SIZE),
                head_block(rows, HEAD_SIZE),
            ],
        ),
        out_shape=[
            jax.ShapeDtypeStruct((rows, kv_heads * heads), jnp.bfloat16),
            jax.ShapeDtypeStruct((rows, kv_heads * heads), jnp.float32),
            jax.ShapeDtypeStruct((kv_heads * group, rows, span), jnp.bfloat16),
            jax.ShapeDtypeStruct((rows, kv_heads * heads), jnp.bfloat16),
            jax.ShapeDtypeStruct((rows, kv_heads * HEAD_SIZE), jnp.bfloat16),
            jax.ShapeDtypeStruct((rows, kv_heads * HEAD_SIZE), jnp.bfloat16),
        ],
        cost_estimate=pl.CostEstimate(
            flops=20 * pairs * HEAD_SIZE, bytes_accessed=rows * width * 8, transcendentals=pairs
        ),
        name="attend_fwd",
    )(slots, pre, *tables)


def attention_backward(
    slots, pre, gated_grad, saved, cos, sin, gains, tile, window, kv_heads, group
):
    rows, width = pre.shape
    heads = group * HEAD_SIZE
    span = (window + 1) * tile
    pairs = kv_heads * group * rows * span
    return pl.pallas_call(
        functools.partial(
            backward_kernel, tile=tile, window=window, kv_heads=kv_heads, group=group
        ),
        grid_spec=pltpu.PrefetchScalarGridSpec(
            num_scalar_prefetch=1,
            grid=(kv_heads,),
            in_specs=[
                whole_block((rows, width)),
                head_block(rows, heads),
                head_block(rows, heads),
                pl.BlockSpec((group, rows, span), lambda head, slots: (head, 0, 0)),
                head_block(rows, heads),
                head_block(rows, HEAD_SIZE),
                head_block(rows, HEAD_SIZE),
                whole_block((rows, HEAD_SIZE)),
                whole_block((rows, HEAD_SIZE)),
                whole_block((1, HEAD_SIZE)),
                whole_block((1, HEAD_SIZE)),
            ],
            out_specs=[whole_block((rows, width))]
            + [pl.BlockSpec((1, 1, HEAD_SIZE), lambda head, slots: (head, 0, 0))] * 2,
            scratch_shapes=[
                pltpu.VMEM((rows, HEAD_SIZE), jnp.float32),
                pltpu.VMEM((rows, HEAD_SIZE), jnp.float32),
            ],
        ),
        out_shape=[
            jax.ShapeDtypeStruct((rows, width), jnp.bfloat16),
            jax.ShapeDtypeStruct((kv_heads, 1, HEAD_SIZE), jnp.float32),
            jax.ShapeDtypeStruct((kv_heads, 1, HEAD_SIZE), jnp.float32),
        ],
        cost_estimate=pl.CostEstimate(
            flops=40 * pairs * HEAD_SIZE, bytes_accessed=rows * width * 16, transcendentals=pairs
        ),
        name="attend_bwd",
    )(slots, pre, gated_grad, *saved, cos, sin, *gains)


def shards(
    block_input,
    out_grad,
    query_proj,
    key_projection,
    value_projection,
    outgate_proj,
    output_proj,
    ffgate_proj,
    ffup_proj,
    ffdown_proj,
    attn_gain,
    ffn_gain,
    query_gain,
    key_gain,
    piece_order,
    doc_ids,
):
    seq_devices = lax.axis_size("seq")
    micro_count, _, local_len, feature_dim = block_input.shape
    full_len = local_len * seq_devices
    piece_len = full_len // piece_order.shape[2]
    query_width = query_proj.shape[1]
    key_width = key_projection.shape[1]
    hidden_width = ffgate_proj.shape[1]
    query_heads = query_width // HEAD_SIZE
    kv_heads = key_width // HEAD_SIZE
    heads_per_group = query_heads // kv_heads
    window = -(-(full_len // 2 - 1) // piece_len)
    micros = range(micro_count)
    place = lax.axis_index("seq")
    chunk = local_len // piece_len
    owners = place ^ jnp.arange(seq_devices) if seq_devices == 4 else jnp.arange(seq_devices)

    attn_gains, ffn_gains, documents = zip(
        *(lax.optimization_barrier((attn_gain, ffn_gain, doc_ids[m, 0])) for m in micros)
    )
    inputs = [block_input[m, 0].astype(jnp.float32) for m in micros]
    scale_one = [rms_scale(x) for x in inputs]
    first_normalized = [x * s for x, s in zip(inputs, scale_one)]
    attn_rows = [
        gather_tokens((x * attn_gains[m]).astype(jnp.bfloat16))
        for m, x in enumerate(first_normalized)
    ]
    qkvg_full = gather_weight(
        jnp.concatenate([query_proj, key_projection, value_projection, outgate_proj], 1)
    )
    output_full = gather_weight(output_proj.T)
    gate_up_full = gather_weight(jnp.concatenate([ffgate_proj, ffup_proj], 1))
    down_full = gather_weight(ffdown_proj.T)
    cot_rows = [gather_tokens(out_grad[m, 0], relayed=m == 0) for m in micros]

    cosines, sines = rope_tables(jnp.arange(full_len, dtype=jnp.int32), HEAD_SIZE)
    sines = sines * jnp.where(jnp.arange(HEAD_SIZE) < HEAD_SIZE // 2, -1.0, 1.0)
    attention = dict(tile=piece_len, window=window, kv_heads=kv_heads, group=heads_per_group)
    kept = []
    middle, scale_two, normed_two, ffn_rows = [], [], [], []
    for m in micros:
        pre = dense(attn_rows[m], qkvg_full)
        held = piece_order[m, 0].reshape(seq_devices, chunk)[owners].reshape(-1)
        at = jnp.arange(held.shape[0], dtype=jnp.int32)
        slots = jnp.sum(jnp.where(held[None, :] == at[:, None], at[None, :], 0), axis=1)
        tables = (
            cosines,
            sines,
            documents[m][:, None],
            documents[m][None, :],
            query_gain[None, :],
            key_gain[None, :],
        )
        gated_low, *saved = attention_forward(slots, pre, tables, **attention)
        part = times_transposed(gated_low, output_full)
        branch = scatter_tokens(part, relayed=True)
        held = (block_input, branch) + tuple(normed_two[-1:])
        held, branch = lax.optimization_barrier(held)[:2]
        now = held[m, 0].astype(jnp.float32) + branch
        middle.append(now)
        scale_two.append(rms_scale(now))
        normed_two.append(now * scale_two[m])
        ffn_rows.append(gather_tokens((normed_two[m] * ffn_gains[m]).astype(jnp.bfloat16)))
        kept.append((slots, pre, saved, tables, gated_low))

    hidden, gate_ffn, up_ffn = [], [], []
    for m in micros:
        gate_up = dense(ffn_rows[m], gate_up_full)
        low = (jax.nn.silu(gate_up[:, :hidden_width]) * gate_up[:, hidden_width:]).astype(
            jnp.bfloat16
        )
        low, gate_up = lax.optimization_barrier((low, gate_up))
        hidden.append(low)
        gate_ffn.append(gate_up[:, :hidden_width])
        up_ffn.append(gate_up[:, hidden_width:])
    down_grad = scatter_weight(outer_sum(cot_rows, hidden))
    outputs, gate_grad, up_grad, ffn_in_grad = [], [], [], []
    for m in micros:
        hidden_grad = dense(cot_rows[m], down_full)
        gate_sigm = jax.nn.sigmoid(gate_ffn[m])
        gate_grad.append(
            (
                hidden_grad * up_ffn[m] * gate_sigm * (1.0 + gate_ffn[m] * (1.0 - gate_sigm))
            ).astype(jnp.bfloat16)
        )
        up_grad.append((hidden_grad * (gate_ffn[m] * gate_sigm)).astype(jnp.bfloat16))
        part = times_transposed(up_grad[m], gate_up_full[:, hidden_width:])
        part = times_transposed(gate_grad[m], gate_up_full[:, :hidden_width]) + rounded(part)
        ffn_in_grad.append(scatter_tokens(part, relayed=True))
    gate_w_grad = scatter_weight(outer_sum(ffn_rows, gate_grad))
    up_w_grad = scatter_weight(outer_sum(ffn_rows, up_grad))
    middle_grad, branch_rows, ffn_gain_sum = [], [], 0.0
    for m in micros:
        held = (out_grad, ffn_in_grad[m]) + tuple(middle_grad[-1:])
        held, ffn_in_grad[m] = lax.optimization_barrier(held)[:2]
        middle_grad.append(
            held[m, 0].astype(jnp.float32)
            + rms_back(ffn_in_grad[m], normed_two[m], scale_two[m], ffn_gains[m])
        )
        middle_grad[m], middle[m] = lax.optimization_barrier((middle_grad[m], middle[m]))
        ffn_gain_sum = ffn_gain_sum + jnp.sum(ffn_in_grad[m] * normed_two[m], axis=0)
        branch_rows.append(gather_tokens(middle_grad[m].astype(jnp.bfloat16)))
    for m in micros:
        part = times_transposed(hidden[m], down_full)
        outputs.append((middle[m] + scatter_tokens(part, relayed=True)).astype(jnp.bfloat16))
    output_grad = scatter_weight(outer_sum(branch_rows, [held[-1] for held in kept]))

    down_grad = down_grad.T
    output_grad = output_grad.T
    query_gain_sum, key_gain_sum, attn_gain_sum = 0.0, 0.0, 0.0
    pre_grads = []
    input_grads = []
    for m in micros:
        slots, pre, saved, tables, gated_low = kept[m]
        gated_grad = dense(branch_rows[m], output_full)
        pre_grad, query_sums, key_sums = attention_backward(
            slots, pre, gated_grad, saved, *tables[:2], tables[-2:], **attention
        )
        query_gain_sum = query_gain_sum + jnp.sum(query_sums, axis=(0, 1))
        key_gain_sum = key_gain_sum + jnp.sum(key_sums, axis=(0, 1))
        attn_in_grad = scatter_tokens(times_transposed(pre_grad, qkvg_full), relayed=True)
        held = (block_input, attn_in_grad) + tuple(input_grads[-1:])
        held, attn_in_grad = lax.optimization_barrier(held)[:2]
        back_normed = held[m, 0].astype(jnp.float32) * scale_one[m]
        pre_grads.append(pre_grad)
        input_grads.append(
            (
                middle_grad[m]
                + rms_back(attn_in_grad, back_normed, scale_one[m], attn_gains[m])
            ).astype(jnp.bfloat16)
        )
        attn_gain_sum = attn_gain_sum + jnp.sum(attn_in_grad * back_normed, axis=0)
    qkvg_grad = scatter_weight(outer_sum(attn_rows, pre_grads))
    cuts = [query_width, query_width + key_width, query_width + 2 * key_width]
    query_w_grad, key_w_grad, value_w_grad, outgate_w_grad = jnp.split(qkvg_grad, cuts, axis=1)
    gains = sum_everywhere(
        jnp.concatenate([attn_gain_sum, ffn_gain_sum, query_gain_sum, key_gain_sum])
    )
    return (
        jnp.stack(outputs)[:, None],
        jnp.stack(input_grads)[:, None],
        query_w_grad,
        key_w_grad,
        value_w_grad,
        outgate_w_grad,
        output_grad,
        gate_w_grad,
        up_w_grad,
        down_grad,
        gains[:feature_dim],
        gains[feature_dim : 2 * feature_dim],
        gains[2 * feature_dim : 2 * feature_dim + HEAD_SIZE],
        gains[2 * feature_dim + HEAD_SIZE :],
    )


def solution(mesh):
    return jax.shard_map(
        shards,
        mesh=mesh,
        in_specs=(
            P(None, "fsdp", "seq", None),
            P(None, "fsdp", "seq", None),
            P("fsdp", "seq"),
            P("fsdp", "seq"),
            P("fsdp", "seq"),
            P("fsdp", "seq"),
            P("seq", "fsdp"),
            P("fsdp", "seq"),
            P("fsdp", "seq"),
            P("seq", "fsdp"),
            P(),
            P(),
            P(),
            P(),
            P(None, "fsdp", None),
            P(None, "fsdp", None),
        ),
        out_specs=(
            P(None, "fsdp", "seq", None),
            P(None, "fsdp", "seq", None),
            P("fsdp", "seq"),
            P("fsdp", "seq"),
            P("fsdp", "seq"),
            P("fsdp", "seq"),
            P("seq", "fsdp"),
            P("fsdp", "seq"),
            P("fsdp", "seq"),
            P("seq", "fsdp"),
            P(),
            P(),
            P(),
            P(),
        ),
        check_vma=False,
    )
```

```python
import functools
import math

import jax
import jax.numpy as jnp
from jax import lax
from jax.experimental import pallas as pl
from jax.experimental.pallas import tpu as pltpu
from jax.sharding import PartitionSpec as P


HEAD_SIZE = 128


EPSILON = 1e-06
ROPE_BASE = 5000000.0


def rms_scale(values):
    return lax.rsqrt(jnp.mean(values * values, axis=-1, keepdims=True) + EPSILON)


def rms_back(grad_out, normed, scales, gain):
    scaled_grad = grad_out * gain
    return scales * (scaled_grad - normed * jnp.mean(scaled_grad * normed, axis=-1, keepdims=True))


def rope_tables(positions, head_dim):
    half_dim = head_dim // 2
    inverse = jnp.exp(
        -math.log(ROPE_BASE) * 2.0 * jnp.arange(half_dim, dtype=jnp.float32) / head_dim
    )
    angles = positions.astype(jnp.float32)[:, None] * inverse[None, :]
    cosines = jnp.cos(angles)
    sines = jnp.sin(angles)
    return (jnp.concatenate([cosines, cosines], -1), jnp.concatenate([sines, sines], -1))


def dense(left, right):
    return jnp.dot(left, right, preferred_element_type=jnp.float32)


def flips(count, bit):
    return [(index, index ^ bit) for index in range(count)]


def gather_tokens(own, relayed=True):
    count = lax.axis_size("seq")
    if count != 4:
        return lax.all_gather(own, "seq", axis=0, tiled=True)
    if not relayed:
        others = [lax.ppermute(own, "seq", flips(4, bit)) for bit in (1, 2, 3)]
        return jnp.concatenate([own] + others, 0)
    half = own.shape[0] // 2
    across = lax.ppermute(own, "seq", flips(4, 1))
    along = lax.ppermute(own, "seq", flips(4, 2))
    far_top, far_bottom = along[:half], across[half:]
    far_top = lax.ppermute(far_top, "seq", flips(4, 1))
    far_bottom = lax.ppermute(far_bottom, "seq", flips(4, 2))
    return jnp.concatenate([own, across, along, far_top, far_bottom], 0)


def scatter_tokens(part, relayed=False):
    count = lax.axis_size("seq")
    low = part.astype(jnp.bfloat16)
    if count != 4:
        return lax.psum_scatter(low, "seq", scatter_dimension=0, tiled=True).astype(jnp.float32)
    rows = part.shape[0] // 4
    own, across, along, far = (low[index * rows : (index + 1) * rows] for index in range(4))
    if not relayed:
        parts = [
            lax.ppermute(piece, "seq", flips(4, bit))
            for bit, piece in ((1, across), (2, along), (3, far))
        ]
        return sum((piece.astype(jnp.float32) for piece in parts), own.astype(jnp.float32))
    half = rows // 2
    relay_top = lax.ppermute(far[:half], "seq", flips(4, 1))
    relay_bottom = lax.ppermute(far[half:], "seq", flips(4, 2))

    def plus(left, right, before):
        right = jnp.pad(right.astype(jnp.float32), ((before, half - before), (0, 0)))
        return (left.astype(jnp.float32) + right).astype(jnp.bfloat16)

    to_across = plus(across, relay_bottom, half)
    to_along = plus(along, relay_top, 0)
    from_across = lax.ppermute(to_across, "seq", flips(4, 1))
    from_along = lax.ppermute(to_along, "seq", flips(4, 2))
    return (
        own.astype(jnp.float32) + from_across.astype(jnp.float32) + from_along.astype(jnp.float32)
    )


def sum_everywhere(value):
    for axis in ("seq", "fsdp"):
        count = lax.axis_size(axis)
        if count & (count - 1):
            value = lax.psum(value, axis)
            continue
        terms = [value] + [lax.ppermute(value, axis, flips(count, bit)) for bit in range(1, count)]
        while len(terms) > 1:
            terms = [terms[at] + terms[at + 1] for at in range(0, len(terms), 2)]
        value = terms[0]
    return value


def gather_weight(shard):
    return lax.all_gather(shard, "fsdp", axis=0, tiled=True)


def scatter_weight(total):
    low = total.astype(jnp.bfloat16)
    low = lax.psum_scatter(low, "fsdp", scatter_dimension=0, tiled=True)
    return low.astype(jnp.float32)


def times_transposed(left, right):
    return jnp.einsum("re,de->rd", left, right, preferred_element_type=jnp.float32)


def rounded(value):
    return value.astype(jnp.bfloat16).astype(jnp.float32)


def outer_sum(lefts, rights):
    total = None
    for m in range(len(lefts)):
        part = outer(lefts[m], rights[m])
        total = part if total is None else part + rounded(total)
    return total


def outer(left, right):
    return jnp.einsum("rd,rf->df", left, right, preferred_element_type=jnp.float32)


def turn(values):
    return pltpu.roll(values, HEAD_SIZE // 2, 1)


def unit(values):
    scale = lax.rsqrt(jnp.mean(values * values, axis=-1, keepdims=True) + EPSILON)
    return values * scale, scale


def window_mask(doc_col_ref, doc_row_ref, begin, low, high):
    same = doc_col_ref[begin:high, :] == doc_row_ref[:, low:high]
    query_at = lax.broadcasted_iota(jnp.int32, same.shape, 0) + begin
    key_at = lax.broadcasted_iota(jnp.int32, same.shape, 1) + low
    return same & (key_at <= query_at)


def dot_last(left, right):
    return lax.dot_general(
        left, right, (((1,), (1,)), ((), ())), preferred_element_type=jnp.float32
    )


def dot_first(left, right):
    return lax.dot_general(
        left, right, (((0,), (0,)), ((), ())), preferred_element_type=jnp.float32
    )


def column(start, index, width):
    return pl.ds(pl.multiple_of(start + index * width, HEAD_SIZE), width)


def head_columns(kv_heads, group):
    at = pl.program_id(0)
    wide = group * HEAD_SIZE
    starts = [head * HEAD_SIZE for head in range(group)]
    keys = kv_heads * wide
    values = keys + kv_heads * HEAD_SIZE
    gates = values + kv_heads * HEAD_SIZE
    spots = [pl.ds(pl.multiple_of(start + at * wide, HEAD_SIZE), HEAD_SIZE) for start in starts]
    spots.append(column(keys, at, HEAD_SIZE))
    spots.append(column(values, at, HEAD_SIZE))
    spots.extend(
        pl.ds(pl.multiple_of(gates + start + at * wide, HEAD_SIZE), HEAD_SIZE) for start in starts
    )
    return spots


def load_heads(
    spots, slots, pre_ref, cos_ref, sin_ref, query_gain_ref, key_gain_ref, q_s, k_s, v_s, tile, group
):
    for at in range(pre_ref.shape[0] // tile):
        rows = pl.ds(pl.multiple_of(slots[at] * tile, tile), tile)
        here = slice(at * tile, (at + 1) * tile)
        cosine, sine = cos_ref[here, :], sin_ref[here, :]
        for head in range(group + 1):
            normed, _ = unit(pre_ref[rows, spots[head]])
            scaled = normed * (query_gain_ref if head < group else key_gain_ref)[...]
            turned = (scaled * cosine + turn(scaled) * sine).astype(jnp.bfloat16)
            if head < group:
                q_s[here, head * HEAD_SIZE : (head + 1) * HEAD_SIZE] = turned
            else:
                k_s[here, :] = turned
        v_s[here, :] = pre_ref[rows, spots[group + 1]].astype(jnp.bfloat16)


def stacked(ref, begin, high, group):
    return jnp.concatenate(
        [ref[begin:high, head * HEAD_SIZE : (head + 1) * HEAD_SIZE] for head in range(group)], 0
    )


def forward_kernel(
    slots,
    pre_ref,
    cos_ref,
    sin_ref,
    doc_col_ref,
    doc_row_ref,
    query_gain_ref,
    key_gain_ref,
    gated_ref,
    attn_ref,
    prob_ref,
    q_s,
    k_s,
    v_s,
    *,
    tile,
    window,
    kv_heads,
    group,
):
    spots = head_columns(kv_heads, group)
    factor = HEAD_SIZE ** (-0.5) * math.log2(math.e)
    load_heads(
        spots, slots, pre_ref, cos_ref, sin_ref, query_gain_ref, key_gain_ref, q_s, k_s, v_s, tile, group
    )
    for at in range(pre_ref.shape[0] // tile):
        begin, high = at * tile, (at + 1) * tile
        low = max(0, at - window) * tile
        mask = window_mask(doc_col_ref, doc_row_ref, begin, low, high)
        rows = pl.ds(pl.multiple_of(slots[at] * tile, tile), tile)
        queries = stacked(q_s, begin, high, group)
        scores = dot_last(queries, k_s[low:high, :]).reshape(group, tile, high - low)
        weights = jnp.where(mask[None], jnp.exp2(scores * factor), 0.0)
        total = jnp.sum(weights, axis=-1, keepdims=True)
        probs = (weights * (1.0 / total)).astype(jnp.bfloat16)
        prob_ref[:, begin:high, : high - low] = probs
        outs = jnp.dot(
            probs.reshape(group * tile, high - low),
            v_s[low:high, :],
            preferred_element_type=jnp.float32,
        )
        for head in range(group):
            cut = slice(head * HEAD_SIZE, (head + 1) * HEAD_SIZE)
            out = outs[head * tile : (head + 1) * tile, :]
            gate_pre = pre_ref[rows, spots[group + 2 + head]]
            gated_ref[rows, cut] = (out * jax.nn.sigmoid(gate_pre)).astype(jnp.bfloat16)
            attn_ref[begin:high, cut] = out


def backward_kernel(
    slots,
    pre_ref,
    grad_ref,
    attn_ref,
    prob_ref,
    q_ref,
    k_ref,
    v_ref,
    cos_ref,
    sin_ref,
    query_gain_ref,
    key_gain_ref,
    out_ref,
    query_sum_ref,
    key_sum_ref,
    dk_s,
    dv_s,
    *,
    tile,
    window,
    kv_heads,
    group,
):
    spots = head_columns(kv_heads, group)
    score_scale = HEAD_SIZE ** (-0.5)
    count = pre_ref.shape[0] // tile
    dk_s[...] = jnp.zeros_like(dk_s)
    dv_s[...] = jnp.zeros_like(dv_s)

    def back(turned_grad, at, rows, head, gain):
        here = slice(at * tile, (at + 1) * tile)
        straight = turned_grad * cos_ref[here, :] - turn(turned_grad) * sin_ref[here, :]
        normed, scale = unit(pre_ref[rows, spots[head]])
        scaled = straight * gain
        shared = jnp.mean(scaled * normed, axis=-1, keepdims=True)
        out_ref[rows, spots[head]] = (
            scale * (scaled - normed * shared)
        ).astype(jnp.bfloat16)
        return jnp.sum(straight * normed, axis=0, keepdims=True)

    query_sum = jnp.zeros((1, HEAD_SIZE), jnp.float32)
    for at in range(count):
        begin, high = at * tile, (at + 1) * tile
        low = max(0, at - window) * tile
        rows = pl.ds(pl.multiple_of(slots[at] * tile, tile), tile)
        for head in range(group):
            cut = slice(head * HEAD_SIZE, (head + 1) * HEAD_SIZE)
            gate_sig = jax.nn.sigmoid(pre_ref[rows, spots[group + 2 + head]])
            gated_grad = grad_ref[rows, cut]
            attn_out = attn_ref[begin:high, cut]
            out_low = (gated_grad * gate_sig).astype(jnp.bfloat16)
            out_ref[rows, spots[group + 2 + head]] = (
                gated_grad * attn_out * gate_sig * (1.0 - gate_sig)
            ).astype(jnp.bfloat16)
            delta = jnp.sum(out_low.astype(jnp.float32) * attn_out, axis=-1, keepdims=True)
            probs = prob_ref[head, begin:high, : high - low]
            prob_grad = dot_last(out_low, v_ref[low:high, :])
            score_grad = (probs.astype(jnp.float32) * (prob_grad - delta)).astype(jnp.bfloat16)
            query_grad = jnp.dot(
                score_grad, k_ref[low:high, :], preferred_element_type=jnp.float32
            )
            dk_s[low:high, :] += dot_first(score_grad, q_ref[begin:high, cut])
            dv_s[low:high, :] += dot_first(probs, out_low)
            query_sum = query_sum + back(
                query_grad * score_scale, at, rows, head, query_gain_ref[...]
            )
    query_sum_ref[0] = query_sum
    key_sum = jnp.zeros((1, HEAD_SIZE), jnp.float32)
    for at in range(count):
        here = slice(at * tile, (at + 1) * tile)
        rows = pl.ds(pl.multiple_of(slots[at] * tile, tile), tile)
        key_sum = key_sum + back(
            dk_s[here, :] * score_scale, at, rows, group, key_gain_ref[...]
        )
        out_ref[rows, spots[group + 1]] = dv_s[
            here, :
        ].astype(jnp.bfloat16)
    key_sum_ref[0] = key_sum


def whole_block(shape):
    return pl.BlockSpec(shape, lambda head, slots: (0,) * len(shape))


def head_block(rows, width):
    return pl.BlockSpec((rows, width), lambda head, slots: (0, head))


def attention_forward(slots, pre, tables, tile, window, kv_heads, group):
    rows, width = pre.shape
    heads = group * HEAD_SIZE
    span = (window + 1) * tile
    pairs = kv_heads * group * rows * span
    return pl.pallas_call(
        functools.partial(
            forward_kernel, tile=tile, window=window, kv_heads=kv_heads, group=group
        ),
        grid_spec=pltpu.PrefetchScalarGridSpec(
            num_scalar_prefetch=1,
            grid=(kv_heads,),
            in_specs=[
                whole_block((rows, width)),
                whole_block((rows, HEAD_SIZE)),
                whole_block((rows, HEAD_SIZE)),
                whole_block((rows, 1)),
                whole_block((1, rows)),
                whole_block((1, HEAD_SIZE)),
                whole_block((1, HEAD_SIZE)),
            ],
            out_specs=[
                head_block(rows, heads),
                head_block(rows, heads),
                pl.BlockSpec((group, rows, span), lambda head, slots: (head, 0, 0)),
                head_block(rows, heads),
                head_block(rows, HEAD_SIZE),
                head_block(rows, HEAD_SIZE),
            ],
        ),
        out_shape=[
            jax.ShapeDtypeStruct((rows, kv_heads * heads), jnp.bfloat16),
            jax.ShapeDtypeStruct((rows, kv_heads * heads), jnp.float32),
            jax.ShapeDtypeStruct((kv_heads * group, rows, span), jnp.bfloat16),
            jax.ShapeDtypeStruct((rows, kv_heads * heads), jnp.bfloat16),
            jax.ShapeDtypeStruct((rows, kv_heads * HEAD_SIZE), jnp.bfloat16),
            jax.ShapeDtypeStruct((rows, kv_heads * HEAD_SIZE), jnp.bfloat16),
        ],
        cost_estimate=pl.CostEstimate(
            flops=20 * pairs * HEAD_SIZE, bytes_accessed=rows * width * 8, transcendentals=pairs
        ),
        name="attend_fwd",
    )(slots, pre, *tables)


def attention_backward(
    slots, pre, gated_grad, saved, cos, sin, gains, tile, window, kv_heads, group
):
    rows, width = pre.shape
    heads = group * HEAD_SIZE
    span = (window + 1) * tile
    pairs = kv_heads * group * rows * span
    return pl.pallas_call(
        functools.partial(
            backward_kernel, tile=tile, window=window, kv_heads=kv_heads, group=group
        ),
        grid_spec=pltpu.PrefetchScalarGridSpec(
            num_scalar_prefetch=1,
            grid=(kv_heads,),
            in_specs=[
                whole_block((rows, width)),
                head_block(rows, heads),
                head_block(rows, heads),
                pl.BlockSpec((group, rows, span), lambda head, slots: (head, 0, 0)),
                head_block(rows, heads),
                head_block(rows, HEAD_SIZE),
                head_block(rows, HEAD_SIZE),
                whole_block((rows, HEAD_SIZE)),
                whole_block((rows, HEAD_SIZE)),
                whole_block((1, HEAD_SIZE)),
                whole_block((1, HEAD_SIZE)),
            ],
            out_specs=[whole_block((rows, width))]
            + [pl.BlockSpec((1, 1, HEAD_SIZE), lambda head, slots: (head, 0, 0))] * 2,
            scratch_shapes=[
                pltpu.VMEM((rows, HEAD_SIZE), jnp.float32),
                pltpu.VMEM((rows, HEAD_SIZE), jnp.float32),
            ],
        ),
        out_shape=[
            jax.ShapeDtypeStruct((rows, width), jnp.bfloat16),
            jax.ShapeDtypeStruct((kv_heads, 1, HEAD_SIZE), jnp.float32),
            jax.ShapeDtypeStruct((kv_heads, 1, HEAD_SIZE), jnp.float32),
        ],
        cost_estimate=pl.CostEstimate(
            flops=40 * pairs * HEAD_SIZE, bytes_accessed=rows * width * 16, transcendentals=pairs
        ),
        name="attend_bwd",
    )(slots, pre, gated_grad, *saved, cos, sin, *gains)


def shards(
    block_input,
    out_grad,
    query_proj,
    key_projection,
    value_projection,
    outgate_proj,
    output_proj,
    ffgate_proj,
    ffup_proj,
    ffdown_proj,
    attn_gain,
    ffn_gain,
    query_gain,
    key_gain,
    piece_order,
    doc_ids,
):
    seq_devices = lax.axis_size("seq")
    micro_count, _, local_len, feature_dim = block_input.shape
    full_len = local_len * seq_devices
    piece_len = full_len // piece_order.shape[2]
    query_width = query_proj.shape[1]
    key_width = key_projection.shape[1]
    hidden_width = ffgate_proj.shape[1]
    query_heads = query_width // HEAD_SIZE
    kv_heads = key_width // HEAD_SIZE
    heads_per_group = query_heads // kv_heads
    window = -(-(full_len // 2 - 1) // piece_len)
    micros = range(micro_count)
    place = lax.axis_index("seq")
    chunk = local_len // piece_len
    owners = place ^ jnp.arange(seq_devices) if seq_devices == 4 else jnp.arange(seq_devices)

    attn_gains, ffn_gains, documents = zip(
        *(lax.optimization_barrier((attn_gain, ffn_gain, doc_ids[m, 0])) for m in micros)
    )
    inputs = [block_input[m, 0].astype(jnp.float32) for m in micros]
    scale_one = [rms_scale(x) for x in inputs]
    first_normalized = [x * s for x, s in zip(inputs, scale_one)]
    attn_rows = [
        gather_tokens((x * attn_gains[m]).astype(jnp.bfloat16))
        for m, x in enumerate(first_normalized)
    ]
    qkvg_full = gather_weight(
        jnp.concatenate([query_proj, key_projection, value_projection, outgate_proj], 1)
    )
    output_full = gather_weight(output_proj.T)
    gate_up_full = gather_weight(jnp.concatenate([ffgate_proj, ffup_proj], 1))
    down_full = gather_weight(ffdown_proj.T)
    cot_rows = [gather_tokens(out_grad[m, 0], relayed=m == 0) for m in micros]

    cosines, sines = rope_tables(jnp.arange(full_len, dtype=jnp.int32), HEAD_SIZE)
    sines = sines * jnp.where(jnp.arange(HEAD_SIZE) < HEAD_SIZE // 2, -1.0, 1.0)
    attention = dict(tile=piece_len, window=window, kv_heads=kv_heads, group=heads_per_group)
    kept = []
    middle, scale_two, normed_two, ffn_rows = [], [], [], []
    for m in micros:
        pre = dense(attn_rows[m], qkvg_full)
        held = piece_order[m, 0].reshape(seq_devices, chunk)[owners].reshape(-1)
        at = jnp.arange(held.shape[0], dtype=jnp.int32)
        slots = jnp.sum(jnp.where(held[None, :] == at[:, None], at[None, :], 0), axis=1)
        tables = (
            cosines,
            sines,
            documents[m][:, None],
            documents[m][None, :],
            query_gain[None, :],
            key_gain[None, :],
        )
        gated_low, *saved = attention_forward(slots, pre, tables, **attention)
        part = times_transposed(gated_low, output_full)
        branch = scatter_tokens(part, relayed=True)
        held = (block_input, branch) + tuple(normed_two[-1:])
        held, branch = lax.optimization_barrier(held)[:2]
        now = held[m, 0].astype(jnp.float32) + branch
        middle.append(now)
        scale_two.append(rms_scale(now))
        normed_two.append(now * scale_two[m])
        ffn_rows.append(gather_tokens((normed_two[m] * ffn_gains[m]).astype(jnp.bfloat16)))
        kept.append((slots, pre, saved, tables, gated_low))

    hidden, gate_ffn, up_ffn = [], [], []
    for m in micros:
        gate_up = dense(ffn_rows[m], gate_up_full)
        low = (jax.nn.silu(gate_up[:, :hidden_width]) * gate_up[:, hidden_width:]).astype(
            jnp.bfloat16
        )
        low, gate_up = lax.optimization_barrier((low, gate_up))
        hidden.append(low)
        gate_ffn.append(gate_up[:, :hidden_width])
        up_ffn.append(gate_up[:, hidden_width:])
    down_grad = scatter_weight(outer_sum(cot_rows, hidden))
    outputs, gate_grad, up_grad, ffn_in_grad = [], [], [], []
    for m in micros:
        hidden_grad = dense(cot_rows[m], down_full)
        gate_sigm = jax.nn.sigmoid(gate_ffn[m])
        gate_grad.append(
            (
                hidden_grad * up_ffn[m] * gate_sigm * (1.0 + gate_ffn[m] * (1.0 - gate_sigm))
            ).astype(jnp.bfloat16)
        )
        up_grad.append((hidden_grad * (gate_ffn[m] * gate_sigm)).astype(jnp.bfloat16))
        part = times_transposed(up_grad[m], gate_up_full[:, hidden_width:])
        part = times_transposed(gate_grad[m], gate_up_full[:, :hidden_width]) + rounded(part)
        ffn_in_grad.append(scatter_tokens(part, relayed=True))
    gate_w_grad = scatter_weight(outer_sum(ffn_rows, gate_grad))
    up_w_grad = scatter_weight(outer_sum(ffn_rows, up_grad))
    middle_grad, branch_rows, ffn_gain_sum = [], [], 0.0
    for m in micros:
        held = (out_grad, ffn_in_grad[m]) + tuple(middle_grad[-1:])
        held, ffn_in_grad[m] = lax.optimization_barrier(held)[:2]
        middle_grad.append(
            held[m, 0].astype(jnp.float32)
            + rms_back(ffn_in_grad[m], normed_two[m], scale_two[m], ffn_gains[m])
        )
        middle_grad[m], middle[m] = lax.optimization_barrier((middle_grad[m], middle[m]))
        ffn_gain_sum = ffn_gain_sum + jnp.sum(ffn_in_grad[m] * normed_two[m], axis=0)
        branch_rows.append(gather_tokens(middle_grad[m].astype(jnp.bfloat16)))
    for m in micros:
        part = times_transposed(hidden[m], down_full)
        outputs.append((middle[m] + scatter_tokens(part, relayed=m > 0)).astype(jnp.bfloat16))
    output_grad = scatter_weight(outer_sum(branch_rows, [held[-1] for held in kept]))

    down_grad = down_grad.T
    output_grad = output_grad.T
    query_gain_sum, key_gain_sum, attn_gain_sum = 0.0, 0.0, 0.0
    pre_grads = []
    input_grads = []
    for m in micros:
        slots, pre, saved, tables, gated_low = kept[m]
        gated_grad = dense(branch_rows[m], output_full)
        pre_grad, query_sums, key_sums = attention_backward(
            slots, pre, gated_grad, saved, *tables[:2], tables[-2:], **attention
        )
        query_gain_sum = query_gain_sum + jnp.sum(query_sums, axis=(0, 1))
        key_gain_sum = key_gain_sum + jnp.sum(key_sums, axis=(0, 1))
        attn_in_grad = scatter_tokens(times_transposed(pre_grad, qkvg_full), relayed=True)
        held = (block_input, attn_in_grad) + tuple(input_grads[-1:])
        held, attn_in_grad = lax.optimization_barrier(held)[:2]
        back_normed = held[m, 0].astype(jnp.float32) * scale_one[m]
        pre_grads.append(pre_grad)
        input_grads.append(
            (
                middle_grad[m]
                + rms_back(attn_in_grad, back_normed, scale_one[m], attn_gains[m])
            ).astype(jnp.bfloat16)
        )
        attn_gain_sum = attn_gain_sum + jnp.sum(attn_in_grad * back_normed, axis=0)
    qkvg_grad = scatter_weight(outer_sum(attn_rows, pre_grads))
    cuts = [query_width, query_width + key_width, query_width + 2 * key_width]
    query_w_grad, key_w_grad, value_w_grad, outgate_w_grad = jnp.split(qkvg_grad, cuts, axis=1)
    gains = sum_everywhere(
        jnp.concatenate([attn_gain_sum, ffn_gain_sum, query_gain_sum, key_gain_sum])
    )
    return (
        jnp.stack(outputs)[:, None],
        jnp.stack(input_grads)[:, None],
        query_w_grad,
        key_w_grad,
        value_w_grad,
        outgate_w_grad,
        output_grad,
        gate_w_grad,
        up_w_grad,
        down_grad,
        gains[:feature_dim],
        gains[feature_dim : 2 * feature_dim],
        gains[2 * feature_dim : 2 * feature_dim + HEAD_SIZE],
        gains[2 * feature_dim + HEAD_SIZE :],
    )


def solution(mesh):
    return jax.shard_map(
        shards,
        mesh=mesh,
        in_specs=(
            P(None, "fsdp", "seq", None),
            P(None, "fsdp", "seq", None),
            P("fsdp", "seq"),
            P("fsdp", "seq"),
            P("fsdp", "seq"),
            P("fsdp", "seq"),
            P("seq", "fsdp"),
            P("fsdp", "seq"),
            P("fsdp", "seq"),
            P("seq", "fsdp"),
            P(),
            P(),
            P(),
            P(),
            P(None, "fsdp", None),
            P(None, "fsdp", None),
        ),
        out_specs=(
            P(None, "fsdp", "seq", None),
            P(None, "fsdp", "seq", None),
            P("fsdp", "seq"),
            P("fsdp", "seq"),
            P("fsdp", "seq"),
            P("fsdp", "seq"),
            P("seq", "fsdp"),
            P("fsdp", "seq"),
            P("fsdp", "seq"),
            P("seq", "fsdp"),
            P(),
            P(),
            P(),
            P(),
        ),
        check_vma=False,
    )
```
